32 devices in a mesh: gx: 2 (over y), gy: 4 (over x, core), gz: 4 (over z).
Axes of the slice: x: 2, y: 2, z: 4, core: 2. Of those that a mesh axis runs over, the one named last changes fastest.
Arguments:
- log_range: float32 [64, 128, 512], P('gx', 'gy', 'gz'), may hold values from 0.7 to 2
- state: float32 [2, 64, 128, 512], P(None, 'gx', 'gy', 'gz'), may hold values from -60 to 60, as said below
- adjoint_start: float32 [2, 64, 128, 512], P(None, 'gx', 'gy', 'gz'), may hold values from -0.3 to 0.3
- obs_index: int32 [2, 2, 4, 4, 4096], P(None, 'gx', 'gy', 'gz'), may hold values from 0 to 131071
- obs_value: float32 [2, 2, 4, 4, 4096], P(None, 'gx', 'gy', 'gz'), may hold values from -6 to 6
Outputs:
- gradient: float32 [64, 128, 512], P('gx', 'gy', 'gz')
- adjoint: float32 [2, 64, 128, 512], P(None, 'gx', 'gy', 'gz')
The draws below stay inside these ranges and needn't reach their ends.
Inputs may be any that keep to these rules, and one draw needn't show every extreme that they name: `obs_index`: each entry numbers a cell of its own device's block as (a * 32 + b) * 128 + c; cells may repeat. `state`: real values.
All inputs are finite; a program needn't handle non-finite values.
Results may differ from the reference program's by a relative error of at most 0.0001.
Values sent between devices are 32-bit elements; how exact they have to be, the bound alone decides.
A program may use at most 320 MiB of HBM per device.

```python
import jax
import jax.numpy as jnp

CX = 32
CY = 32
CZ = 128
NOBS = 4096
REPS = 2
ITERS = 4
NX = 64
NY = 128
NZ = 512
N_GX = 2
N_GY = 4
N_GZ = 4


def draw_state(key, part):
    along_x = (jnp.arange(NX, dtype=jnp.float32) / NX).reshape(-1, 1, 1)
    along_y = (jnp.arange(NY, dtype=jnp.float32) / NY).reshape(1, -1, 1)
    along_z = (jnp.arange(NZ, dtype=jnp.float32) / NZ).reshape(1, 1, -1)
    base = jnp.clip(jax.random.normal(key, (REPS, NX, NY, NZ), jnp.float32), -6.0, 6.0)
    spread = 3.0 ** along_x * 1.7 ** along_y * 1.7 ** along_z
    return base * spread[None]


def place_ends(drawn, rng, smallest, top_value):
    longest = drawn.shape.index(max(drawn.shape))
    spots = []
    for shift in (0, 1):
        where = [jax.random.randint(jax.random.fold_in(rng, axis), (), 0, length) for axis, length in enumerate(drawn.shape)]
        where[longest] = (where[longest] + shift) % drawn.shape[longest]
        spots.append(tuple(where))
    return drawn.at[spots[0]].set(smallest).at[spots[1]].set(top_value)


def block_levels(stream_key, dims, split, low, largest):
    level = 1.0
    for dim, blocks in split:
        draws = jax.random.uniform(jax.random.fold_in(jax.random.fold_in(stream_key, 6), dim), (blocks,), jnp.float32, low / len(split), largest / len(split))
        level = level * jnp.repeat(jnp.exp(draws), dims[dim] // blocks).reshape((-1,) + (1,) * (len(dims) - 1 - dim))
    return level


def scatter_about(rng, extent, deviation, limit, shards=(), kind=jnp.bfloat16):
    entries = deviation * jax.random.normal(rng, extent, jnp.float32)
    if shards:
        entries = entries * block_levels(rng, extent, shards, -0.22, 0.18)
    return jnp.clip(entries, -limit, limit).astype(kind)


def setup_inputs(seed: int = 0) -> dict:
    keys = jax.random.split(jax.random.key(seed), 6)
    log_range = jnp.clip(0.7 + 1.3 * jax.random.uniform(keys[0], (NX, NY, NZ), jnp.float32) ** block_levels(keys[0], (NX, NY, NZ), ((0, 2), (1, 4), (2, 4)), -0.2, 0.2), 0.7, 2.0)
    state = draw_state(jax.random.fold_in(keys[5], 71), 0)
    adjoint_start = scatter_about(keys[2], (REPS, NX, NY, NZ), 0.05, 0.3, ((1, 2), (2, 4), (3, 4)), jnp.float32)
    obs_index = place_ends(jax.random.randint(keys[3], (REPS, N_GX, N_GY, N_GZ, NOBS), 0, CX * CY * CZ), jax.random.fold_in(keys[3], 1), 0, (CX * CY * CZ) - 1).astype(jnp.int32)
    obs_value = scatter_about(keys[4], (REPS, N_GX, N_GY, N_GZ, NOBS), 1.0, 6.0, ((1, 2), (2, 4), (3, 4)), jnp.float32)
    return {"log_range": log_range, "state": state, "adjoint_start": adjoint_start, "obs_index": obs_index, "obs_value": obs_value}


noise_var = 0.25


def stencil(field, kappa_sq):
    beside = jnp.roll(field, -1, 0) + jnp.roll(field, 1, 0)
    beside = beside + jnp.roll(field, -1, 1) + jnp.roll(field, 1, 1)
    beside = beside + jnp.roll(field, -1, 2) + jnp.roll(field, 1, 2)
    return (kappa_sq + 6.0) * field - beside


def reference(log_range, state, adjoint_start, obs_index, obs_value):
    kappa_sq = 4.0 * jnp.exp(-2.0 * log_range)
    block_x = (jnp.arange(N_GX, dtype=jnp.int32) * CX).reshape(-1, 1, 1, 1)
    block_y = (jnp.arange(N_GY, dtype=jnp.int32) * CY).reshape(1, -1, 1, 1)
    block_z = (jnp.arange(N_GZ, dtype=jnp.int32) * CZ).reshape(1, 1, -1, 1)
    total = NX * NY * NZ
    gradient = jnp.zeros((NX, NY, NZ), jnp.float32)
    adjoints = []
    for replica in range(REPS):
        local = obs_index[replica].astype(jnp.int32)
        first = local // (CY * CZ) + block_x
        second = (local // CZ) % CY + block_y
        third = local % CZ + block_z
        global_cell = ((first * NY + second) * NZ + third).reshape(-1).astype(jnp.int32)
        field = state[replica]
        misfit = field.reshape(-1)[global_cell] - obs_value[replica].reshape(-1)
        obs_weight = jnp.zeros((total,), jnp.float32).at[global_cell].add(1.0 / noise_var).reshape(NX, NY, NZ)
        right_side = jnp.zeros((total,), jnp.float32).at[global_cell].add(-misfit / noise_var).reshape(NX, NY, NZ)

        def system(vector):
            return stencil(stencil(vector, kappa_sq), kappa_sq) + obs_weight * vector

        adjoint = adjoint_start[replica]
        residual = right_side - system(adjoint)
        direction = residual
        norm_now = jnp.sum(residual * residual)
        for iteration in range(ITERS):
            image = system(direction)
            step_size = norm_now / jnp.sum(direction * image)
            adjoint = adjoint + step_size * direction
            if iteration + 1 < ITERS:
                residual = residual - step_size * image
                norm_next = jnp.sum(residual * residual)
                direction = residual + (norm_next / norm_now) * direction
                norm_now = norm_next
        state_image = stencil(field, kappa_sq)
        adjoint_image = stencil(adjoint, kappa_sq)
        gradient = gradient + (-2.0 * kappa_sq * (adjoint * state_image + adjoint_image * field))
        adjoints.append(adjoint)
    return gradient, jnp.stack(adjoints, 0)
```

```python
import functools
import itertools

import jax
import jax.numpy as jnp
from jax import lax
from jax.experimental import pallas as pl
from jax.experimental.pallas import tpu as pltpu
from jax.sharding import PartitionSpec as P

ITERS = 4
LANES = 128
HALF = LANES // 2
GHOST = 2
PAD = 8
AXES = ("gx", "gy", "gz")
MESH = pl.DeviceIdType.MESH
UNROLL = 8
X0, R0, W0, W1, W2, STATE, KAP, FIELDS = range(8)
DEEP = (X0, R0, W0, W1)
COPIES = 24

noise_var = 0.25


def kernel(
    sizes, dims, lr_ref, state_ref, start_ref, idx_ref, val_ref, grad_ref, adj_ref,
    ext, uext, ysend, yrecv, zsend, zrecv, zown, xysend, xyrecv, xzsend, xzrecv,
    ck, cp, xe, uz, kz, kap, hot, cols, raw, weight, rhs, z, s_buf, r, ar, q, ast, d, ad, xs, axs,
    xn, rn, dn, gx, gr, gd, red_out, red, send_sem, recv_sem, red_send, red_recv,
):
    sets, cx, cy, cz, nobs = dims
    pitch = cy + PAD
    slabs = cx + 2 * GHOST
    block = slabs * pitch
    lines = cx * cy
    groups = cy // 8
    place = [lax.axis_index(axis) for axis in AXES]
    rank = (place[0] * sizes[1] + place[1]) * sizes[2] + place[2]
    total = sizes[0] * sizes[1] * sizes[2]
    offsets = [o for o in itertools.product(*[range(n) for n in sizes]) if any(o)]

    def device_at(offset):
        return tuple(lax.rem(p + o % n, n) for p, o, n in zip(place, offset, sizes))

    barrier = pltpu.get_barrier_semaphore()
    for offset in offsets:
        pl.semaphore_signal(barrier, inc=1, device_id=device_at(offset), device_id_type=MESH)

    def lanes(rows):
        return lax.broadcasted_iota(jnp.int32, (rows, LANES), 1)

    def roll(v, n):
        n = n % LANES if isinstance(n, int) else n
        return v if isinstance(n, int) and n == 0 else pltpu.roll(v, n, 1)

    def back(x):
        return lax.rem(2 * LANES - 2 * x - 1, LANES)

    low = lanes(1) < HALF
    odd = lanes(1) % 2 == 1
    first = lanes(1) % HALF == 0
    end = lanes(1) % HALF == HALF - 1
    slot = lanes(cy) % HALF // 2

    def at(k, slab, row=0):
        return k * block + slab * pitch + row

    def inner(k, x):
        return pl.ds(pl.multiple_of(at(k, x + GHOST, PAD), 8), cy)

    def dense(k, x):
        return pl.ds(pl.multiple_of((k * cx + x) * cy, 8), cy)

    def plain(x):
        return pl.ds(pl.multiple_of(x * cy, 8), cy)

    def fold(v):
        return jnp.sum(v.reshape(groups, 8, LANES), axis=0)

    def sweep(body, pack=0, sums=0, unroll=UNROLL):
        zero = jnp.zeros((cy, LANES), jnp.float32)

        def step(x, carry):
            faces, gathered = carry
            (even_z, odd_z), terms = body(x)
            mixed = (jnp.where(first, even_z, odd_z), jnp.where(first, odd_z, even_z))[:pack] if pack else ()
            faces = tuple(jnp.where(slot == x, roll(m, 2 * x + 1), f) for m, f in zip(mixed, faces))
            return faces, tuple(a + fold(t) for a, t in zip(gathered, terms))

        start = (zero,) * pack, (jnp.zeros((8, LANES), jnp.float32),) * sums
        return lax.fori_loop(0, cx, step, start, unroll=unroll)

    def copies(e):
        deep = e in DEEP
        out = []

        def add(offset, src, dst):
            n = len(out)
            out.append(pltpu.make_async_remote_copy(
                src_ref=src, dst_ref=dst, send_sem=send_sem.at[e, n], recv_sem=recv_sem.at[e, n],
                device_id=device_at(offset), device_id_type=MESH))

        add((0, 0, -1), zsend.at[e, 0], zrecv.at[e, 0, PAD:PAD + cy])
        add((0, 0, 1), zsend.at[e, 1], zrecv.at[e, 1, PAD:PAD + cy])
        for k in range(2):
            for j in range(GHOST) if deep else (0,):
                add((-1, 0, 0), ext.at[e, pl.ds(at(k, GHOST + j, PAD), cy)],
                    ext.at[e, pl.ds(at(k, GHOST + cx + j, PAD), cy)])
                add((1, 0, 0), ext.at[e, pl.ds(at(k, GHOST + cx - 1 - j, PAD), cy)],
                    ext.at[e, pl.ds(at(k, GHOST - 1 - j, PAD), cy)])
        planes = slice(0, GHOST if deep else 1)
        for side in range(2):
            add((0, 2 * side - 1, 0), ysend.at[e, side, planes], yrecv.at[e, side, planes])
        if deep:
            for n, (a, b) in enumerate(itertools.product((-1, 1), repeat=2)):
                add((a, b, 0), xysend.at[e, n], xyrecv.at[e, n])
                add((a, 0, b), xzsend.at[e, n], xzrecv.at[e, n])
                tile = slice(0, 8) if a < 0 else slice(cy - 8, cy)
                into = slice(PAD + cy, 2 * PAD + cy) if a < 0 else slice(0, PAD)
                add((0, a, b), zsend.at[e, (b + 1) // 2, tile], zrecv.at[e, (b + 1) // 2, into])
        return out

    def send(e, faces):
        zown[e] = faces[0]
        if e in DEEP:
            zsend[e, 0] = jnp.where(odd, faces[0], roll(faces[1], -1))
            zsend[e, 1] = jnp.where(odd, roll(faces[1], 1), faces[0])
        else:
            zsend[e, 0] = faces[0]
            zsend[e, 1] = faces[0]
        for side in range(2):
            for plane in range(GHOST if e in DEEP else 1):
                y = cy - 1 - plane if side else plane
                for k in range(2):
                    ysend[e, side, plane, k * cx:(k + 1) * cx] = ext[e, pl.ds(at(k, GHOST, PAD + y), cx, stride=pitch), :]
        if e in DEEP:
            for n, (a, b) in enumerate(itertools.product((-1, 1), repeat=2)):
                for k in range(2):
                    row = at(k, GHOST + (cx - 1 if a > 0 else 0), PAD + (cy - 1 if b > 0 else 0))
                    xysend[e, n, k:k + 1] = ext[e, row:row + 1, :]
                lane = (2 * (cx - 1) if a > 0 else 0) + (0 if b > 0 else 1)
                packed = jnp.zeros((8, LANES), jnp.float32)
                for g in range(groups):
                    part = roll(zsend[e, (b + 1) // 2, 8 * g:8 * g + 8], 2 * g)
                    packed = jnp.where(lanes(8) % HALF == (lane + 2 * g) % HALF, part, packed)
                xzsend[e, n] = packed
        for copy in copies(e):
            copy.start()

    def arrive(e):
        for copy in copies(e):
            copy.wait()
        for side in range(2):
            for plane in range(GHOST if e in DEEP else 1):
                for k in range(2):
                    row = at(k, GHOST, PAD - 1 - plane if side else pitch + plane)
                    ext[e, pl.ds(row, cx, stride=pitch), :] = yrecv[e, side, plane, k * cx:(k + 1) * cx]
        if e not in DEEP:
            left, right = zrecv[e, 1, PAD:PAD + cy], zrecv[e, 0, PAD:PAD + cy]
            cp[PAD:] = jnp.where(odd, roll(left, HALF + 1), roll(right, HALF - 1))
            return
        left, right = zrecv[e, 1], zrecv[e, 0]
        ck[...] = jnp.where(odd, roll(left, HALF + 1), roll(right, HALF - 1))
        side_x = [[None, None], [None, None]]
        for n, (a, b) in enumerate(itertools.product((-1, 1), repeat=2)):
            for k in range(2):
                row = at(k, GHOST - 1 if a > 0 else GHOST + cx, PAD - 1 if b > 0 else pitch)
                ext[e, row:row + 1, :] = xyrecv[e, n, k:k + 1]
            lane = (2 * (cx - 1) if a > 0 else 0) + (0 if b > 0 else 1)
            shift = -(lane + HALF) if b > 0 else HALF - 1 - lane
            side_x[0 if a > 0 else 1][0 if b > 0 else 1] = [
                roll(xzrecv[e, n], shift - 2 * g) for g in range(groups)]
        for side in range(2):
            for g in range(groups):
                xe[side, 8 * g:8 * g + 8] = jnp.where(first, side_x[side][0][g], side_x[side][1][g])
        top = lax.broadcasted_iota(jnp.int32, (PAD, LANES), 0) == 0
        cp[0:PAD] = jnp.where(top, roll(ck[PAD + cy:], 2), ck[0:PAD])
        mid = ck[PAD:PAD + cy]
        cp[PAD:] = mid
        around = jnp.where(odd, roll(left[PAD:PAD + cy], HALF), roll(right[PAD:PAD + cy], HALF)) + zown[e]
        pos = lanes(1) % HALF
        around = around + jnp.where(pos < 2, roll(xe[0], 1), roll(mid, 2))
        around = around + jnp.where((pos >= 2 * cx - 2) & (pos < 2 * cx), roll(xe[1], 2 * cx - 1), roll(mid, -2))
        around = around + (ck[PAD - 1:PAD + cy - 1] + ck[PAD + 1:PAD + cy + 1])
        uz[...] = kz[...] * mid - around

    def apply(src, base, rows, edge):
        bases = [pl.multiple_of(base + k * block, 8) for k in range(2)]
        center = [src[pl.ds(b, rows), :] for b in bases]
        beside = [
            center[1] + jnp.where(first, edge, roll(center[1], 1)),
            center[0] + jnp.where(end, edge, roll(center[0], -1)),
        ]
        out = []
        for k, b in enumerate(bases):
            around = src[pl.ds(b + pitch, rows), :] + src[pl.ds(b - pitch, rows), :]
            around = around + (src[pl.ds(b + 1, rows), :] + src[pl.ds(b - 1, rows), :])
            out.append(ext[KAP, pl.ds(b, rows), :] * center[k] - (around + beside[k]))
        return out

    def wide(e):
        src, dst = ext.at[e], uext.at[e]

        def put(base, rows, edge):
            for k, v in enumerate(apply(src, base, rows, edge)):
                dst[pl.ds(pl.multiple_of(base + k * block, 8), rows), :] = v

        put(at(0, GHOST - 1, PAD), cy, xe[0])

        def step(x, carry):
            put(at(0, x + GHOST), pitch, roll(cp[...], back(x)))
            return carry
        lax.fori_loop(0, cx, step, 0, unroll=UNROLL)
        put(at(0, GHOST + cx, PAD), cy, xe[1])
        put(at(0, GHOST + cx), PAD, roll(cp[0:PAD], -2 * cx - 1))

    def again(e, x):
        return apply(uext.at[e], at(0, x + GHOST, PAD), cy, roll(uz[...], back(x)))

    def once(e, x):
        return apply(ext.at[e], at(0, x + GHOST, PAD), cy, roll(cp[PAD:], back(x)))

    def reduce_start(n, gathered):
        line = jnp.zeros((1, LANES), jnp.float32)
        for j, acc in enumerate(gathered):
            part = jnp.sum(acc, axis=0, keepdims=True)
            for s in range(sets):
                value = jnp.sum(jnp.where(low == (s == 0), part, 0.0), axis=1, keepdims=True)
                line = jnp.where(lanes(1) == 2 * s + j, value, line)
        red_out[n] = line
        red[n, rank] = line
        for offset in offsets:
            pltpu.make_async_remote_copy(
                src_ref=red_out.at[n], dst_ref=red.at[n, rank], send_sem=red_send.at[n],
                recv_sem=red_recv.at[n], device_id=device_at(offset), device_id_type=MESH).start()

    def spread(v, j):
        value = jnp.sum(jnp.where(lanes(1) == j, v, 0.0), axis=1, keepdims=True)
        return jnp.broadcast_to(value, (1, LANES))

    def reduce_end(n):
        many = red.at[n, pl.ds(0, total - 1)]
        pltpu.make_async_copy(many, many, red_recv.at[n]).wait()
        pltpu.make_async_copy(many, many, red_send.at[n]).wait()
        line = jnp.sum(red[n], axis=0)
        return [jnp.where(low, spread(line, j), spread(line, 2 + j)) for j in range(2)]

    def take(v, index):
        return jnp.take_along_axis(v, index, axis=1)

    lane = lanes(cy)
    split_low = 2 * (lane % HALF) + lane // HALF
    split_high = 2 * (lane % HALF) + 1 - lane // HALF
    join_low = lane // 2 + HALF * (lane % 2)
    join_high = lane // 2 + HALF * (1 - lane % 2)

    def split(ref, x):
        a, b = take(ref[0, plain(x), :], split_low), take(ref[1, plain(x), :], split_high)
        return jnp.where(low, a, b), roll(jnp.where(low, b, a), HALF)

    def join(even_z, odd_z):
        turned = roll(odd_z, HALF)
        return take(jnp.where(low, even_z, turned), join_low), take(jnp.where(low, turned, even_z), join_high)

    def keep(e, x, pair):
        for k in range(2):
            ext[e, inner(k, x), :] = pair[k]

    def load(e, ref):
        def body(x):
            pair = split(ref, x)
            keep(e, x, pair)
            return pair, ()
        return sweep(body, 2 if e in DEEP else 1)[0]

    def load_kap(x):
        value = 4.0 * jnp.exp(-2.0 * lr_ref[plain(x), :])
        kap[plain(x), :] = value
        a = take(value + 6.0, split_low)
        b = roll(a, HALF)
        pair = jnp.where(low, a, b), jnp.where(low, b, a)
        keep(KAP, x, pair)
        return pair, ()

    faces_start = load(X0, start_ref)
    faces_kap = sweep(load_kap, 1)[0]
    pl.semaphore_wait(barrier, total - 1)
    send(X0, faces_start)
    send(KAP, faces_kap)
    send(STATE, load(STATE, state_ref))

    upper = lines // 2
    for s in range(sets):
        cell = idx_ref[s]
        value = val_ref[s]
        top = value.astype(jnp.bfloat16).astype(jnp.float32)
        line = cell // cz
        key = line // upper * LANES + cell % cz
        col = lax.broadcasted_iota(jnp.int32, (2 * LANES, nobs), 0)
        half = col % LANES // HALF
        hit = key == col // LANES * LANES + 2 * (col % HALF) + (half if s == 0 else 1 - half)
        cols[0] = jnp.where(hit, 1.0, 0.0).astype(jnp.bfloat16)
        cols[1] = jnp.where(hit, top, 0.0).astype(jnp.bfloat16)
        cols[2] = jnp.where(hit, value - top, 0.0).astype(jnp.bfloat16)
        short = line % upper

        def rows_of(m, carry, short=short):
            ids = lax.broadcasted_iota(jnp.int32, (LANES, nobs), 0) + m * LANES
            hot[pl.ds(pl.multiple_of(m * LANES, LANES), LANES), :] = jnp.where(ids == short, 1.0, 0.0).astype(jnp.bfloat16)
            return carry
        lax.fori_loop(0, upper // LANES, rows_of, 0)

        def product(n):
            return lax.dot_general(hot[...], cols[n], (((1,), (1,)), ((), ())), preferred_element_type=jnp.float32)

        count = product(0) * (1.0 / noise_var)
        amount = (product(1) + product(2)) * (1.0 / noise_var)
        for h in range(2):
            raw[s, 0, h * upper:(h + 1) * upper] = count[:, h * LANES:(h + 1) * LANES]
            raw[s, 1, h * upper:(h + 1) * upper] = amount[:, h * LANES:(h + 1) * LANES]

    def mix(n, x):
        a, b = raw[0, n, plain(x), :], raw[1, n, plain(x), :]
        return jnp.where(low, a, b), roll(jnp.where(low, b, a), HALF)

    def right_pass(x):
        count, amount = mix(0, x), mix(1, x)
        for k in range(2):
            weight[dense(k, x), :] = count[k]
            rhs[dense(k, x), :] = amount[k] - count[k] * (ext[STATE, inner(k, x), :] + ext[X0, inner(k, x), :])
        return (None, None), ()

    sweep(right_pass)
    arrive(KAP)
    kz[...] = cp[PAD:]
    arrive(X0)
    wide(X0)

    def residual_pass(x):
        out = again(X0, x)
        pair = [rhs[dense(k, x), :] - out[k] for k in range(2)]
        keep(R0, x, pair)
        return pair, ()

    send(R0, sweep(residual_pass, 2)[0])

    arrive(STATE)

    def state_pass(x):
        out = once(STATE, x)
        for k in range(2):
            ast[dense(k, x), :] = out[k]
        return (None, None), ()

    sweep(state_pass)

    arrive(R0)
    wide(R0)

    def image_pass(x):
        out = again(R0, x)
        now = [ext[R0, inner(k, x), :] for k in range(2)]
        pair = [out[k] + weight[dense(k, x), :] * now[k] for k in range(2)]
        keep(W0, x, pair)
        return pair, (now[0] * now[0] + now[1] * now[1], now[0] * pair[0] + now[1] * pair[1])

    faces, gathered = sweep(image_pass, 2, 2)
    send(W0, faces)
    reduce_start(0, gathered)

    norms, steps, ratios = [], [], []
    for k, e in enumerate((W0, W1)):
        arrive(e)
        wide(e)

        def next_image(x, e=e):
            out = again(e, x)
            for p in range(2):
                q[dense(p, x), :] = out[p] + weight[dense(p, x), :] * ext[e, inner(p, x), :]
            return (None, None), ()

        sweep(next_image)
        norm, product = reduce_end(k)
        if k == 0:
            ratio, step_size = None, norm / product
        else:
            ratio = norm / norms[-1]
            step_size = norm / (product - ratio * norm / steps[-1])
        norms.append(norm)
        steps.append(step_size)
        ratios.append(ratio)

        def update(x, k=k, e=e, ratio=ratio, step_size=step_size):
            pair, terms = [], []
            for p in range(2):
                here, there = dense(p, x), inner(p, x)
                image, vec = q[here, :], ext[e, there, :]
                if k == 0:
                    z[here, :] = image
                    follow, now = vec, ext[R0, there, :]
                else:
                    image = image + ratio * z[here, :]
                    follow, now = vec + ratio * ext[W0, there, :], r[k - 1, here, :]
                    s_buf[here, :] = follow
                vec = vec - step_size * image
                now = now - step_size * follow
                ext[e + 1, there, :] = vec
                r[k, here, :] = now
                pair.append(vec)
                terms.append((now * now, now * vec))
            return pair, (terms[0][0] + terms[1][0], terms[0][1] + terms[1][1])

        faces, gathered = sweep(update, 2 if e + 1 in DEEP else 1, 2)
        send(e + 1, faces)
        reduce_start(k + 1, gathered)

        def trail(x, k=k, ratio=ratio, step_size=step_size):
            for p in range(2):
                here, there = dense(p, x), inner(p, x)
                if k == 0:
                    xs[here, :] = ext[X0, there, :] + step_size * ext[R0, there, :]
                    now = uext[R0, there, :]
                    axs[here, :] = uext[X0, there, :] + step_size * now
                    ar[0, here, :] = now - step_size * uext[W0, there, :]
                else:
                    toward = r[0, here, :] + ratio * ext[R0, there, :]
                    d[here, :] = toward
                    xs[here, :] = xs[here, :] + step_size * toward
                    now = ar[0, here, :]
                    toward = now + ratio * uext[R0, there, :]
                    ad[here, :] = toward
                    axs[here, :] = axs[here, :] + step_size * toward
                    follow = uext[W1, there, :] + ratio * uext[W0, there, :]
                    q[here, :] = follow
                    ar[1, here, :] = now - step_size * follow
            return (None, None), ()

        sweep(trail)

    arrive(W2)

    def last_half(x):
        out = once(W2, x)
        for p in range(2):
            z[dense(p, x), :] = out[p]
        return (None, None), ()

    sweep(last_half)
    norm, product = reduce_end(2)
    ratio = norm / norms[-1]
    step_size = norm / (product - ratio * norm / steps[-1])

    def last_residual(x):
        norm_terms, terms = [], []
        for p in range(2):
            here, there = dense(p, x), inner(p, x)
            now = r[1, here, :] - step_size * (ext[W2, there, :] + ratio * s_buf[here, :])
            inner_now = ar[1, here, :] - step_size * (z[here, :] + ratio * q[here, :])
            r[2, here, :] = now
            ar[2, here, :] = inner_now
            norm_terms.append(now * now)
            terms.append(inner_now * inner_now + weight[here, :] * now * now)
        return (None, None), (norm_terms[0] + norm_terms[1], terms[0] + terms[1])

    reduce_start(3, sweep(last_residual, 0, 2)[1])

    def prepare(x):
        towards, olds, nows, grads = [], [], [], []
        for p in range(2):
            here, there = dense(p, x), inner(p, x)
            field, image = ext[STATE, there, :], ast[here, :]
            toward = r[1, here, :] + ratio * d[here, :]
            applied = ar[1, here, :] + ratio * ad[here, :]
            old = xs[here, :] + step_size * toward
            old_applied = axs[here, :] + step_size * applied
            now, now_applied = r[2, here, :], ar[2, here, :]
            towards.append(toward)
            olds.append(old)
            nows.append(now)
            grads.append((
                old * image + old_applied * field,
                now * image + now_applied * field,
                toward * image + applied * field,
            ))
        here = plain(x)
        scale = -2.0 * kap[here, :]
        for ref, pair in ((xn, olds), (rn, nows), (dn, towards)):
            for s, v in enumerate(join(*pair)):
                ref[s, here, :] = v
        parts = [join(grads[0][n], grads[1][n]) for n in range(3)]
        gx[here, :] = scale * (parts[0][0] + parts[0][1])
        for s in range(sets):
            gr[s, here, :] = scale * parts[1][s]
            gd[s, here, :] = scale * parts[2][s]
        return (None, None), ()

    sweep(prepare, unroll=4)
    last_norm, last_product = reduce_end(3)
    last_ratio = last_norm / norm
    last_step = last_norm / (last_product - last_ratio * last_norm / step_size)
    last_both = last_step * last_ratio
    one = [spread(last_step, s * HALF) for s in range(sets)]
    two = [spread(last_both, s * HALF) for s in range(sets)]

    def finish(x, carry):
        here = plain(x)
        grad = gx[here, :]
        for s in range(sets):
            adj_ref[s, here, :] = xn[s, here, :] + (one[s] * rn[s, here, :] + two[s] * dn[s, here, :])
            grad = grad + (one[s] * gr[s, here, :] + two[s] * gd[s, here, :])
        grad_ref[here, :] = grad
        return carry
    lax.fori_loop(0, cx, finish, 0, unroll=UNROLL)


def on_device(sizes, log_range, state, adjoint_start, obs_index, obs_value):
    sets, cx, cy, cz = state.shape
    nobs = obs_index.shape[-1]
    rows = cx * cy
    total = sizes[0] * sizes[1] * sizes[2]
    whole = 2 * (cx + 2 * GHOST) * (cy + PAD) + 8
    f32 = jnp.float32
    field = pltpu.VMEM((2 * rows, LANES), f32)
    natural = pltpu.VMEM((sets, rows, cz), f32)
    vmem = pl.BlockSpec(memory_space=pltpu.VMEM)
    gradient, adjoint = pl.pallas_call(
        functools.partial(kernel, sizes, (sets, cx, cy, cz, nobs)),
        out_shape=(
            jax.ShapeDtypeStruct((rows, cz), jnp.float32),
            jax.ShapeDtypeStruct((sets, rows, cz), jnp.float32),
        ),
        in_specs=[vmem] * 5,
        out_specs=(vmem, vmem),
        scratch_shapes=[
            pltpu.VMEM((FIELDS, whole, LANES), f32),
            pltpu.VMEM((len(DEEP), whole, LANES), f32),
            pltpu.VMEM((FIELDS, 2, GHOST, 2 * cx, LANES), f32),
            pltpu.VMEM((FIELDS, 2, GHOST, 2 * cx, LANES), f32),
            pltpu.VMEM((FIELDS, 2, cy, LANES), f32),
            pltpu.VMEM((FIELDS, 2, cy + 2 * PAD, LANES), f32),
            pltpu.VMEM((FIELDS, cy, LANES), f32),
            *[pltpu.VMEM((len(DEEP), 4, 8, LANES), f32)] * 4,
            pltpu.VMEM((cy + 2 * PAD, LANES), f32),
            pltpu.VMEM((cy + PAD, LANES), f32),
            pltpu.VMEM((2, cy, LANES), f32),
            pltpu.VMEM((cy, LANES), f32),
            pltpu.VMEM((cy, LANES), f32),
            pltpu.VMEM((rows, cz), f32),
            pltpu.VMEM((rows // 2, nobs), jnp.bfloat16),
            pltpu.VMEM((3, 2 * LANES, nobs), jnp.bfloat16),
            pltpu.VMEM((sets, 2, rows, LANES), f32),
            field, field, field, field,
            pltpu.VMEM((3, 2 * rows, LANES), f32),
            pltpu.VMEM((3, 2 * rows, LANES), f32),
            *[field] * 6,
            natural, natural, natural,
            pltpu.VMEM((rows, cz), f32),
            natural, natural,
            pltpu.VMEM((ITERS, 1, LANES), f32),
            pltpu.VMEM((ITERS, total, 1, LANES), f32),
            pltpu.SemaphoreType.DMA((FIELDS, COPIES)),
            pltpu.SemaphoreType.DMA((FIELDS, COPIES)),
            pltpu.SemaphoreType.DMA((ITERS,)),
            pltpu.SemaphoreType.DMA((ITERS,)),
        ],
        compiler_params=pltpu.CompilerParams(
            collective_id=0, has_side_effects=True, vmem_limit_bytes=63 * 1024 * 1024
        ),
    )(
        log_range.reshape(rows, cz),
        state.reshape(sets, rows, cz),
        adjoint_start.reshape(sets, rows, cz),
        obs_index.reshape(sets, 1, nobs),
        obs_value.reshape(sets, 1, nobs),
    )
    return gradient.reshape(cx, cy, cz), adjoint.reshape(sets, cx, cy, cz)


def solution(mesh):
    in_specs = (
        P("gx", "gy", "gz"),
        P(None, "gx", "gy", "gz"),
        P(None, "gx", "gy", "gz"),
        P(None, "gx", "gy", "gz", None),
        P(None, "gx", "gy", "gz", None),
    )
    out_specs = (P("gx", "gy", "gz"), P(None, "gx", "gy", "gz"))
    sizes = tuple(mesh.shape[axis] for axis in AXES)
    return jax.shard_map(
        functools.partial(on_device, sizes), mesh=mesh, in_specs=in_specs, out_specs=out_specs, check_vma=False
    )
```

```python
import functools
import itertools

import jax
import jax.numpy as jnp
from jax import lax
from jax.experimental import pallas as pl
from jax.experimental.pallas import tpu as pltpu
from jax.sharding import PartitionSpec as P

ITERS = 4
LANES = 128
HALF = LANES // 2
GHOST = 2
PAD = 8
AXES = ("gx", "gy", "gz")
MESH = pl.DeviceIdType.MESH
UNROLL = 8
X0, R0, W0, W1, W2, STATE, KAP, FIELDS = range(8)
DEEP = (X0, R0, W0, W1)
COPIES = 24

noise_var = 0.25


def kernel(
    sizes, dims, lr_hbm, state_hbm, start_hbm, idx_hbm, val_hbm, grad_ref, adj_ref,
    lr_ref, state_ref, start_ref, idx_ref, val_ref, ext, uext, ysend, yrecv, zsend, zrecv, zown, xysend, xyrecv, xzsend, xzrecv,
    ck, cp, xe, uz, kz, kap, cols, raw, weight, rhs, z, s_buf, r, ar, q, ast, ad, xs, axs,
    gr, gd, red_out, red, send_sem, recv_sem, red_send, red_recv, load_sem,
):
    sets, cx, cy, cz, nobs = dims
    pitch = cy + PAD
    slabs = cx + 2 * GHOST
    block = slabs * pitch
    lines = cx * cy
    groups = cy // 8
    place = [lax.axis_index(axis) for axis in AXES]
    rank = (place[0] * sizes[1] + place[1]) * sizes[2] + place[2]
    total = sizes[0] * sizes[1] * sizes[2]
    offsets = [o for o in itertools.product(*[range(n) for n in sizes]) if any(o)]

    def device_at(offset):
        return tuple(lax.rem(p + o % n, n) for p, o, n in zip(place, offset, sizes))

    barrier = pltpu.get_barrier_semaphore()
    for offset in offsets:
        pl.semaphore_signal(barrier, inc=1, device_id=device_at(offset), device_id_type=MESH)

    pairs = ((start_hbm, start_ref), (idx_hbm, idx_ref), (val_hbm, val_ref), (lr_hbm, lr_ref), (state_hbm, state_ref))
    loads = [pltpu.make_async_copy(a, b, load_sem.at[n]) for n, (a, b) in enumerate(pairs)]
    for copy in loads:
        copy.start()

    def lanes(rows):
        return lax.broadcasted_iota(jnp.int32, (rows, LANES), 1)

    def roll(v, n):
        n = n % LANES if isinstance(n, int) else n
        return v if isinstance(n, int) and n == 0 else pltpu.roll(v, n, 1)

    def back(x):
        return lax.rem(2 * LANES - 2 * x - 1, LANES)

    low = lanes(1) < HALF
    odd = lanes(1) % 2 == 1
    first = lanes(1) % HALF == 0
    end = lanes(1) % HALF == HALF - 1
    slot = lanes(cy) % HALF // 2

    def at(k, slab, row=0):
        return k * block + slab * pitch + row

    def inner(k, x):
        return pl.ds(pl.multiple_of(at(k, x + GHOST, PAD), 8), cy)

    def dense(k, x):
        return pl.ds(pl.multiple_of((k * cx + x) * cy, 8), cy)

    def plain(x):
        return pl.ds(pl.multiple_of(x * cy, 8), cy)

    def fold(v):
        return jnp.sum(v.reshape(groups, 8, LANES), axis=0)

    def sweep(body, pack=0, sums=0, unroll=UNROLL, early=None):
        zero = jnp.zeros((cy, LANES), jnp.float32)

        def step(x, carry):
            faces, gathered = carry
            (even_z, odd_z), terms = body(x)
            mixed = (jnp.where(first, even_z, odd_z), jnp.where(first, odd_z, even_z))[:pack] if pack else ()
            faces = tuple(jnp.where(slot == x, roll(m, 2 * x + 1), f) for m, f in zip(mixed, faces))
            return faces, tuple(a + fold(t) for a, t in zip(gathered, terms))

        start = (zero,) * pack, (jnp.zeros((8, LANES), jnp.float32),) * sums
        if early is None:
            return lax.fori_loop(0, cx, step, start, unroll=unroll)
        for x in (*range(GHOST), *range(cx - GHOST, cx)):
            start = step(x, start)
        send_x(early)
        return lax.fori_loop(GHOST, cx - GHOST, step, start, unroll=7)

    def copies(e):
        deep = e in DEEP
        out = []

        def add(offset, src, dst):
            n = len(out)
            out.append(pltpu.make_async_remote_copy(
                src_ref=src, dst_ref=dst, send_sem=send_sem.at[e, n], recv_sem=recv_sem.at[e, n],
                device_id=device_at(offset), device_id_type=MESH))

        for k in range(2):
            for j in range(GHOST) if deep else (0,):
                add((-1, 0, 0), ext.at[e, pl.ds(at(k, GHOST + j, PAD), cy)],
                    ext.at[e, pl.ds(at(k, GHOST + cx + j, PAD), cy)])
                add((1, 0, 0), ext.at[e, pl.ds(at(k, GHOST + cx - 1 - j, PAD), cy)],
                    ext.at[e, pl.ds(at(k, GHOST - 1 - j, PAD), cy)])
        near = len(out)
        add((0, 0, -1), zsend.at[e, 0], zrecv.at[e, 0, PAD:PAD + cy])
        add((0, 0, 1), zsend.at[e, 1], zrecv.at[e, 1, PAD:PAD + cy])
        planes = slice(0, GHOST if deep else 1)
        for side in range(2):
            add((0, 2 * side - 1, 0), ysend.at[e, side, planes], yrecv.at[e, side, planes])
        if deep:
            for n, (a, b) in enumerate(itertools.product((-1, 1), repeat=2)):
                add((a, b, 0), xysend.at[e, n], xyrecv.at[e, n])
                add((a, 0, b), xzsend.at[e, n], xzrecv.at[e, n])
                tile = slice(0, 8) if a < 0 else slice(cy - 8, cy)
                into = slice(PAD + cy, 2 * PAD + cy) if a < 0 else slice(0, PAD)
                add((0, a, b), zsend.at[e, (b + 1) // 2, tile], zrecv.at[e, (b + 1) // 2, into])
        return out[:near], out[near:]

    def send_x(e):
        for copy in copies(e)[0]:
            copy.start()

    def send(e, faces):
        zown[e] = faces[0]
        if e in DEEP:
            zsend[e, 0] = jnp.where(odd, faces[0], roll(faces[1], -1))
            zsend[e, 1] = jnp.where(odd, roll(faces[1], 1), faces[0])
        else:
            zsend[e, 0] = faces[0]
            zsend[e, 1] = faces[0]
        for side in range(2):
            for plane in range(GHOST if e in DEEP else 1):
                y = cy - 1 - plane if side else plane
                for k in range(2):
                    ysend[e, side, plane, k * cx:(k + 1) * cx] = ext[e, pl.ds(at(k, GHOST, PAD + y), cx, stride=pitch), :]
        if e in DEEP:
            for n, (a, b) in enumerate(itertools.product((-1, 1), repeat=2)):
                for k in range(2):
                    row = at(k, GHOST + (cx - 1 if a > 0 else 0), PAD + (cy - 1 if b > 0 else 0))
                    xysend[e, n, k:k + 1] = ext[e, row:row + 1, :]
                lane = (2 * (cx - 1) if a > 0 else 0) + (0 if b > 0 else 1)
                packed = jnp.zeros((8, LANES), jnp.float32)
                for g in range(groups):
                    part = roll(zsend[e, (b + 1) // 2, 8 * g:8 * g + 8], 2 * g)
                    packed = jnp.where(lanes(8) % HALF == (lane + 2 * g) % HALF, part, packed)
                xzsend[e, n] = packed
        for copy in copies(e)[1]:
            copy.start()

    def arrive(e):
        for copy in sum(copies(e), []):
            copy.wait()
        for side in range(2):
            for plane in range(GHOST if e in DEEP else 1):
                for k in range(2):
                    row = at(k, GHOST, PAD - 1 - plane if side else pitch + plane)
                    ext[e, pl.ds(row, cx, stride=pitch), :] = yrecv[e, side, plane, k * cx:(k + 1) * cx]
        if e not in DEEP:
            left, right = zrecv[e, 1, PAD:PAD + cy], zrecv[e, 0, PAD:PAD + cy]
            cp[PAD:] = jnp.where(odd, roll(left, HALF + 1), roll(right, HALF - 1))
            return
        left, right = zrecv[e, 1], zrecv[e, 0]
        ck[...] = jnp.where(odd, roll(left, HALF + 1), roll(right, HALF - 1))
        side_x = [[None, None], [None, None]]
        for n, (a, b) in enumerate(itertools.product((-1, 1), repeat=2)):
            for k in range(2):
                row = at(k, GHOST - 1 if a > 0 else GHOST + cx, PAD - 1 if b > 0 else pitch)
                ext[e, row:row + 1, :] = xyrecv[e, n, k:k + 1]
            lane = (2 * (cx - 1) if a > 0 else 0) + (0 if b > 0 else 1)
            shift = -(lane + HALF) if b > 0 else HALF - 1 - lane
            side_x[0 if a > 0 else 1][0 if b > 0 else 1] = [
                roll(xzrecv[e, n], shift - 2 * g) for g in range(groups)]
        for side in range(2):
            for g in range(groups):
                xe[side, 8 * g:8 * g + 8] = jnp.where(first, side_x[side][0][g], side_x[side][1][g])
        top = lax.broadcasted_iota(jnp.int32, (PAD, LANES), 0) == 0
        cp[0:PAD] = jnp.where(top, roll(ck[PAD + cy:], 2), ck[0:PAD])
        mid = ck[PAD:PAD + cy]
        cp[PAD:] = mid
        around = jnp.where(odd, roll(left[PAD:PAD + cy], HALF), roll(right[PAD:PAD + cy], HALF)) + zown[e]
        pos = lanes(1) % HALF
        around = around + jnp.where(pos < 2, roll(xe[0], 1), roll(mid, 2))
        around = around + jnp.where((pos >= 2 * cx - 2) & (pos < 2 * cx), roll(xe[1], 2 * cx - 1), roll(mid, -2))
        around = around + (ck[PAD - 1:PAD + cy - 1] + ck[PAD + 1:PAD + cy + 1])
        uz[...] = kz[...] * mid - around

    def apply(src, base, rows, edge):
        bases = [pl.multiple_of(base + k * block, 8) for k in range(2)]
        center = [src[pl.ds(b, rows), :] for b in bases]
        beside = [
            center[1] + jnp.where(first, edge, roll(center[1], 1)),
            center[0] + jnp.where(end, edge, roll(center[0], -1)),
        ]
        out = []
        for k, b in enumerate(bases):
            around = src[pl.ds(b + pitch, rows), :] + src[pl.ds(b - pitch, rows), :]
            around = around + (src[pl.ds(b + 1, rows), :] + src[pl.ds(b - 1, rows), :])
            out.append(ext[KAP, pl.ds(b, rows), :] * center[k] - (around + beside[k]))
        return out

    def wide(e):
        src, dst = ext.at[e], uext.at[e]

        def put(base, rows, edge):
            for k, v in enumerate(apply(src, base, rows, edge)):
                dst[pl.ds(pl.multiple_of(base + k * block, 8), rows), :] = v

        put(at(0, GHOST - 1, PAD), cy, xe[0])

        def step(x, carry):
            put(at(0, x + GHOST), pitch, roll(cp[...], back(x)))
            return carry
        lax.fori_loop(0, cx, step, 0, unroll=UNROLL)
        put(at(0, GHOST + cx, PAD), cy, xe[1])
        put(at(0, GHOST + cx), PAD, roll(cp[0:PAD], -2 * cx - 1))

    def again(e, x):
        return apply(uext.at[e], at(0, x + GHOST, PAD), cy, roll(uz[...], back(x)))

    def once(e, x):
        return apply(ext.at[e], at(0, x + GHOST, PAD), cy, roll(cp[PAD:], back(x)))

    def reduce_start(n, gathered):
        line = jnp.zeros((1, LANES), jnp.float32)
        for j, acc in enumerate(gathered):
            part = jnp.sum(acc, axis=0, keepdims=True)
            for s in range(sets):
                value = jnp.sum(jnp.where(low == (s == 0), part, 0.0), axis=1, keepdims=True)
                line = jnp.where(lanes(1) == 2 * s + j, value, line)
        red_out[n] = line
        red[n, rank] = line
        for offset in offsets:
            pltpu.make_async_remote_copy(
                src_ref=red_out.at[n], dst_ref=red.at[n, rank], send_sem=red_send.at[n],
                recv_sem=red_recv.at[n], device_id=device_at(offset), device_id_type=MESH).start()

    def spread(v, j):
        value = jnp.sum(jnp.where(lanes(1) == j, v, 0.0), axis=1, keepdims=True)
        return jnp.broadcast_to(value, (1, LANES))

    def reduce_end(n):
        many = red.at[n, pl.ds(0, total - 1)]
        pltpu.make_async_copy(many, many, red_recv.at[n]).wait()
        pltpu.make_async_copy(many, many, red_send.at[n]).wait()
        line = jnp.sum(red[n], axis=0)
        return [jnp.where(low, spread(line, j), spread(line, 2 + j)) for j in range(2)]

    def take(v, index):
        return jnp.take_along_axis(v, index, axis=1)

    lane = lanes(cy)
    apart = 2 * (lane % HALF) + lane // HALF
    together = lane // 2 + HALF * (lane % 2)

    def permute(ref, index, rows):
        def step(m, carry):
            here = pl.ds(pl.multiple_of(m * cy, 8), cy)
            ref[here, :] = take(ref[here, :], index)
            return carry
        lax.fori_loop(0, rows // cy, step, 0, unroll=2 * UNROLL)

    def split(ref, x):
        a, b = ref[0, plain(x), :], ref[1, plain(x), :]
        return jnp.where(low, a, roll(b, HALF)), jnp.where(low, roll(a, HALF), b)

    def join(even_z, odd_z):
        return jnp.where(low, even_z, roll(odd_z, HALF)), jnp.where(low, roll(even_z, HALF), odd_z)

    def keep(e, x, pair):
        for k in range(2):
            ext[e, inner(k, x), :] = pair[k]

    def load(e, ref):
        for s in range(sets):
            permute(ref.at[s], apart, lines)

        def body(x):
            pair = split(ref, x)
            keep(e, x, pair)
            return pair, ()
        return sweep(body, 2 if e in DEEP else 1)[0]

    def load_kap(x):
        value = 4.0 * jnp.exp(-2.0 * lr_ref[plain(x), :])
        kap[plain(x), :] = value
        a = value + 6.0
        b = roll(a, HALF)
        pair = jnp.where(low, a, b), jnp.where(low, b, a)
        keep(KAP, x, pair)
        return pair, ()

    upper = lines // 2

    def observe(s):
        cell = idx_ref[s]
        value = val_ref[s]
        top = value.astype(jnp.bfloat16).astype(jnp.float32)
        line = cell // cz
        key = line // upper * LANES + cell % cz
        col = lax.broadcasted_iota(jnp.int32, (2 * LANES, nobs), 0)
        half = col % LANES // HALF
        hit = key == col // LANES * LANES + 2 * (col % HALF) + (half if s == 0 else 1 - half)
        for n, part in enumerate((1.0, top, value - top)):
            cols[2 * LANES * n:2 * LANES * (n + 1)] = jnp.where(hit, part, 0.0).astype(jnp.bfloat16)
        short = line % upper

        def step(m, carry):
            ids = lax.broadcasted_iota(jnp.int32, (upper, nobs), 0) + m * upper
            hot = jnp.where(ids == short, 1.0, 0.0).astype(jnp.bfloat16)
            got = lax.dot_general(hot, cols[...], (((1,), (1,)), ((), ())), preferred_element_type=jnp.float32)
            count = got[:, :2 * LANES] * (1.0 / noise_var)
            amount = (got[:, 2 * LANES:4 * LANES] + got[:, 4 * LANES:]) * (1.0 / noise_var)
            for h in range(2):
                here = pl.ds(pl.multiple_of(m * upper + h * upper, upper), upper)
                raw[s, 0, here, :] = count[:, h * LANES:(h + 1) * LANES]
                raw[s, 1, here, :] = amount[:, h * LANES:(h + 1) * LANES]
            return carry

        lax.fori_loop(0, 1, step, 0)

    loads[0].wait()
    faces_start = load(X0, start_ref)
    loads[1].wait()
    loads[2].wait()
    observe(0)
    loads[3].wait()
    permute(lr_ref, apart, lines)
    faces_kap = sweep(load_kap, 1)[0]
    pl.semaphore_wait(barrier, total - 1)
    send_x(X0)
    send(X0, faces_start)
    send_x(KAP)
    send(KAP, faces_kap)
    loads[4].wait()
    faces_state = load(STATE, state_ref)
    send_x(STATE)
    send(STATE, faces_state)
    observe(1)

    def mix(n, x):
        a, b = raw[0, n, plain(x), :], raw[1, n, plain(x), :]
        return jnp.where(low, a, b), roll(jnp.where(low, b, a), HALF)

    def right_pass(x):
        count, amount = mix(0, x), mix(1, x)
        for k in range(2):
            weight[dense(k, x), :] = count[k]
            rhs[dense(k, x), :] = amount[k] - count[k] * (ext[STATE, inner(k, x), :] + ext[X0, inner(k, x), :])
        return (None, None), ()

    sweep(right_pass)
    arrive(KAP)
    kz[...] = cp[PAD:]
    arrive(X0)
    wide(X0)

    def residual_pass(x):
        out = again(X0, x)
        pair = [rhs[dense(k, x), :] - out[k] for k in range(2)]
        keep(R0, x, pair)
        return pair, ()

    send(R0, sweep(residual_pass, 2, early=R0)[0])

    arrive(STATE)

    def state_pass(x):
        out = once(STATE, x)
        for k in range(2):
            ast[dense(k, x), :] = out[k]
        return (None, None), ()

    sweep(state_pass)

    arrive(R0)
    wide(R0)

    def image_pass(x):
        out = again(R0, x)
        now = [ext[R0, inner(k, x), :] for k in range(2)]
        pair = [out[k] + weight[dense(k, x), :] * now[k] for k in range(2)]
        keep(W0, x, pair)
        return pair, (now[0] * now[0] + now[1] * now[1], now[0] * pair[0] + now[1] * pair[1])

    faces, gathered = sweep(image_pass, 2, 2, early=W0)
    send(W0, faces)
    reduce_start(0, gathered)

    norms, steps, ratios = [], [], []
    for k, e in enumerate((W0, W1)):
        arrive(e)
        wide(e)

        def next_image(x, e=e):
            out = again(e, x)
            for p in range(2):
                q[dense(p, x), :] = out[p] + weight[dense(p, x), :] * ext[e, inner(p, x), :]
            return (None, None), ()

        sweep(next_image)
        norm, product = reduce_end(k)
        if k == 0:
            ratio, step_size = None, norm / product
        else:
            ratio = norm / norms[-1]
            step_size = norm / (product - ratio * norm / steps[-1])
        norms.append(norm)
        steps.append(step_size)
        ratios.append(ratio)

        def update(x, k=k, e=e, ratio=ratio, step_size=step_size):
            pair, terms = [], []
            for p in range(2):
                here, there = dense(p, x), inner(p, x)
                image, vec = q[here, :], ext[e, there, :]
                if k == 0:
                    z[here, :] = image
                    follow, now = vec, ext[R0, there, :]
                else:
                    image = image + ratio * z[here, :]
                    follow, now = vec + ratio * ext[W0, there, :], r[k - 1, here, :]
                    s_buf[here, :] = follow
                vec = vec - step_size * image
                now = now - step_size * follow
                ext[e + 1, there, :] = vec
                r[k, here, :] = now
                pair.append(vec)
                terms.append((now * now, now * vec))
            return pair, (terms[0][0] + terms[1][0], terms[0][1] + terms[1][1])

        faces, gathered = sweep(update, 2 if e + 1 in DEEP else 1, 2, early=e + 1)
        send(e + 1, faces)
        reduce_start(k + 1, gathered)

        def trail(x, k=k, ratio=ratio, step_size=step_size):
            for p in range(2):
                here, there = dense(p, x), inner(p, x)
                if k == 0:
                    xs[here, :] = ext[X0, there, :] + step_size * ext[R0, there, :]
                    now = uext[R0, there, :]
                    axs[here, :] = uext[X0, there, :] + step_size * now
                    ar[0, here, :] = now - step_size * uext[W0, there, :]
                else:
                    toward = r[0, here, :] + ratio * ext[R0, there, :]
                    rhs[here, :] = toward
                    xs[here, :] = xs[here, :] + step_size * toward
                    now = ar[0, here, :]
                    toward = now + ratio * uext[R0, there, :]
                    ad[here, :] = toward
                    axs[here, :] = axs[here, :] + step_size * toward
                    follow = uext[W1, there, :] + ratio * uext[W0, there, :]
                    q[here, :] = follow
                    ar[1, here, :] = now - step_size * follow
            return (None, None), ()

        sweep(trail)

    arrive(W2)

    def last_half(x):
        out = once(W2, x)
        for p in range(2):
            z[dense(p, x), :] = out[p]
        return (None, None), ()

    sweep(last_half)
    norm, product = reduce_end(2)
    ratio = norm / norms[-1]
    step_size = norm / (product - ratio * norm / steps[-1])

    def last_residual(x):
        norm_terms, terms = [], []
        for p in range(2):
            here, there = dense(p, x), inner(p, x)
            now = r[1, here, :] - step_size * (ext[W2, there, :] + ratio * s_buf[here, :])
            inner_now = ar[1, here, :] - step_size * (z[here, :] + ratio * q[here, :])
            r[2, here, :] = now
            ar[2, here, :] = inner_now
            norm_terms.append(now * now)
            terms.append(inner_now * inner_now + weight[here, :] * now * now)
        return (None, None), (norm_terms[0] + norm_terms[1], terms[0] + terms[1])

    reduce_start(3, sweep(last_residual, 0, 2)[1])

    def prepare(x):
        towards, olds, nows, grads = [], [], [], []
        for p in range(2):
            here, there = dense(p, x), inner(p, x)
            field, image = ext[STATE, there, :], ast[here, :]
            toward = r[1, here, :] + ratio * rhs[here, :]
            applied = ar[1, here, :] + ratio * ad[here, :]
            old = xs[here, :] + step_size * toward
            old_applied = axs[here, :] + step_size * applied
            now, now_applied = r[2, here, :], ar[2, here, :]
            towards.append(toward)
            olds.append(old)
            nows.append(now)
            grads.append((
                old * image + old_applied * field,
                now * image + now_applied * field,
                toward * image + applied * field,
            ))
        here = plain(x)
        scale = -2.0 * kap[here, :]
        for s, v in enumerate(join(*olds)):
            adj_ref[s, here, :] = v
        for n, pair in enumerate((nows, towards)):
            for s, v in enumerate(join(*pair)):
                raw[s, n, here, :] = v
        parts = [join(grads[0][n], grads[1][n]) for n in range(3)]
        grad_ref[here, :] = scale * (parts[0][0] + parts[0][1])
        for s in range(sets):
            gr[s, here, :] = scale * parts[1][s]
            gd[s, here, :] = scale * parts[2][s]
        return (None, None), ()

    sweep(prepare, unroll=4)
    for s in range(sets):
        permute(adj_ref.at[s], together, lines)
        for n in range(2):
            permute(raw.at[s, n], together, lines)
        permute(gr.at[s], together, lines)
        permute(gd.at[s], together, lines)
    permute(grad_ref, together, lines)
    last_norm, last_product = reduce_end(3)
    last_ratio = last_norm / norm
    last_step = last_norm / (last_product - last_ratio * last_norm / step_size)
    last_both = last_step * last_ratio
    one = [spread(last_step, s * HALF) for s in range(sets)]
    two = [spread(last_both, s * HALF) for s in range(sets)]

    def finish(x, carry):
        here = plain(x)
        grad = grad_ref[here, :]
        for s in range(sets):
            adj_ref[s, here, :] = adj_ref[s, here, :] + (one[s] * raw[s, 0, here, :] + two[s] * raw[s, 1, here, :])
            grad = grad + (one[s] * gr[s, here, :] + two[s] * gd[s, here, :])
        grad_ref[here, :] = grad
        return carry
    lax.fori_loop(0, cx, finish, 0, unroll=UNROLL)


def on_device(sizes, log_range, state, adjoint_start, obs_index, obs_value):
    sets, cx, cy, cz = state.shape
    nobs = obs_index.shape[-1]
    rows = cx * cy
    total = sizes[0] * sizes[1] * sizes[2]
    whole = 2 * (cx + 2 * GHOST) * (cy + PAD) + 8
    f32 = jnp.float32
    field = pltpu.VMEM((2 * rows, LANES), f32)
    natural = pltpu.VMEM((sets, rows, cz), f32)
    vmem = pl.BlockSpec(memory_space=pltpu.VMEM)
    gradient, adjoint = pl.pallas_call(
        functools.partial(kernel, sizes, (sets, cx, cy, cz, nobs)),
        out_shape=(
            jax.ShapeDtypeStruct((rows, cz), jnp.float32),
            jax.ShapeDtypeStruct((sets, rows, cz), jnp.float32),
        ),
        in_specs=[pl.BlockSpec(memory_space=pltpu.HBM)] * 5,
        out_specs=(vmem, vmem),
        scratch_shapes=[
            pltpu.VMEM((rows, cz), f32),
            natural,
            natural,
            pltpu.VMEM((sets, 1, nobs), jnp.int32),
            pltpu.VMEM((sets, 1, nobs), f32),
            pltpu.VMEM((FIELDS, whole, LANES), f32),
            pltpu.VMEM((len(DEEP), whole, LANES), f32),
            pltpu.VMEM((FIELDS, 2, GHOST, 2 * cx, LANES), f32),
            pltpu.VMEM((FIELDS, 2, GHOST, 2 * cx, LANES), f32),
            pltpu.VMEM((FIELDS, 2, cy, LANES), f32),
            pltpu.VMEM((FIELDS, 2, cy + 2 * PAD, LANES), f32),
            pltpu.VMEM((FIELDS, cy, LANES), f32),
            *[pltpu.VMEM((len(DEEP), 4, 8, LANES), f32)] * 4,
            pltpu.VMEM((cy + 2 * PAD, LANES), f32),
            pltpu.VMEM((cy + PAD, LANES), f32),
            pltpu.VMEM((2, cy, LANES), f32),
            pltpu.VMEM((cy, LANES), f32),
            pltpu.VMEM((cy, LANES), f32),
            pltpu.VMEM((rows, cz), f32),
            pltpu.VMEM((6 * LANES, nobs), jnp.bfloat16),
            pltpu.VMEM((sets, 2, rows, LANES), f32),
            field, field, field, field,
            pltpu.VMEM((3, 2 * rows, LANES), f32),
            pltpu.VMEM((3, 2 * rows, LANES), f32),
            *[field] * 5,
            natural, natural,
            pltpu.VMEM((ITERS, 1, LANES), f32),
            pltpu.VMEM((ITERS, total, 1, LANES), f32),
            pltpu.SemaphoreType.DMA((FIELDS, COPIES)),
            pltpu.SemaphoreType.DMA((FIELDS, COPIES)),
            pltpu.SemaphoreType.DMA((ITERS,)),
            pltpu.SemaphoreType.DMA((ITERS,)),
            pltpu.SemaphoreType.DMA((5,)),
        ],
        compiler_params=pltpu.CompilerParams(
            collective_id=0, has_side_effects=True, vmem_limit_bytes=63 * 1024 * 1024
        ),
    )(
        log_range.reshape(rows, cz),
        state.reshape(sets, rows, cz),
        adjoint_start.reshape(sets, rows, cz),
        obs_index.reshape(sets, 1, nobs),
        obs_value.reshape(sets, 1, nobs),
    )
    return gradient.reshape(cx, cy, cz), adjoint.reshape(sets, cx, cy, cz)


def solution(mesh):
    in_specs = (
        P("gx", "gy", "gz"),
        P(None, "gx", "gy", "gz"),
        P(None, "gx", "gy", "gz"),
        P(None, "gx", "gy", "gz", None),
        P(None, "gx", "gy", "gz", None),
    )
    out_specs = (P("gx", "gy", "gz"), P(None, "gx", "gy", "gz"))
    sizes = tuple(mesh.shape[axis] for axis in AXES)
    return jax.shard_map(
        functools.partial(on_device, sizes), mesh=mesh, in_specs=in_specs, out_specs=out_specs, check_vma=False
    )
```

```python
import functools
import itertools

import jax
import jax.numpy as jnp
from jax import lax
from jax.experimental import pallas as pl
from jax.experimental.pallas import tpu as pltpu
from jax.sharding import PartitionSpec as P

ITERS = 4
LANES = 128
HALF = LANES // 2
GHOST = 2
PAD = 8
AXES = ("gx", "gy", "gz")
MESH = pl.DeviceIdType.MESH
UNROLL = 8
X0, R0, W0, W1, W2, STATE, KAP, FIELDS = range(8)
DEEP = (X0, R0, W0, W1)
COPIES = 24

noise_var = 0.25


def kernel(
    sizes, dims, lr_hbm, state_hbm, start_hbm, idx_hbm, val_hbm, grad_ref, adj_ref,
    lr_ref, state_ref, start_ref, idx_ref, val_ref, ext, uext, ysend, yrecv, zsend, zrecv, zown, xysend, xyrecv, xzsend, xzrecv,
    ck, cp, xe, uz, kz, kap, cols, raw, weight, rhs, z, s_buf, r, ar, q, ast, ad, xs, axs,
    gr, gd, red_out, red, send_sem, recv_sem, red_send, red_recv, load_sem,
):
    sets, cx, cy, cz, nobs = dims
    pitch = cy + PAD
    slabs = cx + 2 * GHOST
    block = slabs * pitch
    lines = cx * cy
    groups = cy // 8
    place = [lax.axis_index(axis) for axis in AXES]
    rank = (place[0] * sizes[1] + place[1]) * sizes[2] + place[2]
    total = sizes[0] * sizes[1] * sizes[2]
    offsets = [o for o in itertools.product(*[range(n) for n in sizes]) if any(o)]

    def device_at(offset):
        return tuple(lax.rem(p + o % n, n) for p, o, n in zip(place, offset, sizes))

    barrier = pltpu.get_barrier_semaphore()
    for offset in offsets:
        pl.semaphore_signal(barrier, inc=1, device_id=device_at(offset), device_id_type=MESH)

    pairs = ((start_hbm, start_ref), (idx_hbm, idx_ref), (val_hbm, val_ref), (lr_hbm, lr_ref), (state_hbm, state_ref))
    loads = [pltpu.make_async_copy(a, b, load_sem.at[n]) for n, (a, b) in enumerate(pairs)]
    for copy in loads:
        copy.start()

    def lanes(rows):
        return lax.broadcasted_iota(jnp.int32, (rows, LANES), 1)

    def roll(v, n):
        n = n % LANES if isinstance(n, int) else n
        return v if isinstance(n, int) and n == 0 else pltpu.roll(v, n, 1)

    def back(x):
        return lax.rem(2 * LANES - 2 * x - 1, LANES)

    low = lanes(1) < HALF
    odd = lanes(1) % 2 == 1
    first = lanes(1) % HALF == 0
    end = lanes(1) % HALF == HALF - 1
    slot = lanes(cy) % HALF // 2

    def at(k, slab, row=0):
        return k * block + slab * pitch + row

    def inner(k, x):
        return pl.ds(pl.multiple_of(at(k, x + GHOST, PAD), 8), cy)

    def dense(k, x):
        return pl.ds(pl.multiple_of((k * cx + x) * cy, 8), cy)

    def plain(x):
        return pl.ds(pl.multiple_of(x * cy, 8), cy)

    def fold(v):
        return jnp.sum(v.reshape(groups, 8, LANES), axis=0)

    def sweep(body, pack=0, sums=0, unroll=UNROLL, early=None):
        zero = jnp.zeros((cy, LANES), jnp.float32)

        def step(x, carry):
            faces, gathered = carry
            (even_z, odd_z), terms = body(x)
            mixed = (jnp.where(first, even_z, odd_z), jnp.where(first, odd_z, even_z))[:pack] if pack else ()
            faces = tuple(jnp.where(slot == x, roll(m, 2 * x + 1), f) for m, f in zip(mixed, faces))
            return faces, tuple(a + fold(t) for a, t in zip(gathered, terms))

        start = (zero,) * pack, (jnp.zeros((8, LANES), jnp.float32),) * sums
        if early is None:
            return lax.fori_loop(0, cx, step, start, unroll=unroll)
        for x in (*range(GHOST), *range(cx - GHOST, cx)):
            start = step(x, start)
        send_x(early)
        return lax.fori_loop(GHOST, cx - GHOST, step, start, unroll=7)

    def copies(e):
        deep = e in DEEP
        out = []

        def add(offset, src, dst):
            n = len(out)
            out.append(pltpu.make_async_remote_copy(
                src_ref=src, dst_ref=dst, send_sem=send_sem.at[e, n], recv_sem=recv_sem.at[e, n],
                device_id=device_at(offset), device_id_type=MESH))

        for k in range(2):
            for j in range(GHOST) if deep else (0,):
                add((-1, 0, 0), ext.at[e, pl.ds(at(k, GHOST + j, PAD), cy)],
                    ext.at[e, pl.ds(at(k, GHOST + cx + j, PAD), cy)])
                add((1, 0, 0), ext.at[e, pl.ds(at(k, GHOST + cx - 1 - j, PAD), cy)],
                    ext.at[e, pl.ds(at(k, GHOST - 1 - j, PAD), cy)])
        near = len(out)
        add((0, 0, -1), zsend.at[e, 0], zrecv.at[e, 0, PAD:PAD + cy])
        add((0, 0, 1), zsend.at[e, 1], zrecv.at[e, 1, PAD:PAD + cy])
        planes = slice(0, GHOST if deep else 1)
        for side in range(2):
            add((0, 2 * side - 1, 0), ysend.at[e, side, planes], yrecv.at[e, side, planes])
        if deep:
            for n, (a, b) in enumerate(itertools.product((-1, 1), repeat=2)):
                add((a, b, 0), xysend.at[e, n], xyrecv.at[e, n])
                add((a, 0, b), xzsend.at[e, n], xzrecv.at[e, n])
                tile = slice(0, 8) if a < 0 else slice(cy - 8, cy)
                into = slice(PAD + cy, 2 * PAD + cy) if a < 0 else slice(0, PAD)
                add((0, a, b), zsend.at[e, (b + 1) // 2, tile], zrecv.at[e, (b + 1) // 2, into])
        return out[:near], out[near:]

    def send_x(e):
        for copy in copies(e)[0]:
            copy.start()

    def send(e, faces):
        zown[e] = faces[0]
        if e in DEEP:
            zsend[e, 0] = jnp.where(odd, faces[0], roll(faces[1], -1))
            zsend[e, 1] = jnp.where(odd, roll(faces[1], 1), faces[0])
        else:
            zsend[e, 0] = faces[0]
            zsend[e, 1] = faces[0]
        for side in range(2):
            for plane in range(GHOST if e in DEEP else 1):
                y = cy - 1 - plane if side else plane
                for k in range(2):
                    ysend[e, side, plane, k * cx:(k + 1) * cx] = ext[e, pl.ds(at(k, GHOST, PAD + y), cx, stride=pitch), :]
        if e in DEEP:
            for n, (a, b) in enumerate(itertools.product((-1, 1), repeat=2)):
                for k in range(2):
                    row = at(k, GHOST + (cx - 1 if a > 0 else 0), PAD + (cy - 1 if b > 0 else 0))
                    xysend[e, n, k:k + 1] = ext[e, row:row + 1, :]
                lane = (2 * (cx - 1) if a > 0 else 0) + (0 if b > 0 else 1)
                packed = jnp.zeros((8, LANES), jnp.float32)
                for g in range(groups):
                    part = roll(zsend[e, (b + 1) // 2, 8 * g:8 * g + 8], 2 * g)
                    packed = jnp.where(lanes(8) % HALF == (lane + 2 * g) % HALF, part, packed)
                xzsend[e, n] = packed
        for copy in copies(e)[1]:
            copy.start()

    def arrive(e):
        for copy in sum(copies(e), []):
            copy.wait()
        for side in range(2):
            for plane in range(GHOST if e in DEEP else 1):
                for k in range(2):
                    row = at(k, GHOST, PAD - 1 - plane if side else pitch + plane)
                    ext[e, pl.ds(row, cx, stride=pitch), :] = yrecv[e, side, plane, k * cx:(k + 1) * cx]
        if e not in DEEP:
            left, right = zrecv[e, 1, PAD:PAD + cy], zrecv[e, 0, PAD:PAD + cy]
            cp[PAD:] = jnp.where(odd, roll(left, HALF + 1), roll(right, HALF - 1))
            return
        left, right = zrecv[e, 1], zrecv[e, 0]
        ck[...] = jnp.where(odd, roll(left, HALF + 1), roll(right, HALF - 1))
        side_x = [[None, None], [None, None]]
        for n, (a, b) in enumerate(itertools.product((-1, 1), repeat=2)):
            for k in range(2):
                row = at(k, GHOST - 1 if a > 0 else GHOST + cx, PAD - 1 if b > 0 else pitch)
                ext[e, row:row + 1, :] = xyrecv[e, n, k:k + 1]
            lane = (2 * (cx - 1) if a > 0 else 0) + (0 if b > 0 else 1)
            shift = -(lane + HALF) if b > 0 else HALF - 1 - lane
            side_x[0 if a > 0 else 1][0 if b > 0 else 1] = [
                roll(xzrecv[e, n], shift - 2 * g) for g in range(groups)]
        for side in range(2):
            for g in range(groups):
                xe[side, 8 * g:8 * g + 8] = jnp.where(first, side_x[side][0][g], side_x[side][1][g])
        top = lax.broadcasted_iota(jnp.int32, (PAD, LANES), 0) == 0
        cp[0:PAD] = jnp.where(top, roll(ck[PAD + cy:], 2), ck[0:PAD])
        mid = ck[PAD:PAD + cy]
        cp[PAD:] = mid
        around = jnp.where(odd, roll(left[PAD:PAD + cy], HALF), roll(right[PAD:PAD + cy], HALF)) + zown[e]
        pos = lanes(1) % HALF
        around = around + jnp.where(pos < 2, roll(xe[0], 1), roll(mid, 2))
        around = around + jnp.where((pos >= 2 * cx - 2) & (pos < 2 * cx), roll(xe[1], 2 * cx - 1), roll(mid, -2))
        around = around + (ck[PAD - 1:PAD + cy - 1] + ck[PAD + 1:PAD + cy + 1])
        uz[...] = kz[...] * mid - around

    def apply(src, base, rows, edge):
        bases = [pl.multiple_of(base + k * block, 8) for k in range(2)]
        center = [src[pl.ds(b, rows), :] for b in bases]
        beside = [
            center[1] + jnp.where(first, edge, roll(center[1], 1)),
            center[0] + jnp.where(end, edge, roll(center[0], -1)),
        ]
        out = []
        for k, b in enumerate(bases):
            around = src[pl.ds(b + pitch, rows), :] + src[pl.ds(b - pitch, rows), :]
            around = around + (src[pl.ds(b + 1, rows), :] + src[pl.ds(b - 1, rows), :])
            out.append(ext[KAP, pl.ds(b, rows), :] * center[k] - (around + beside[k]))
        return out

    def wide(e):
        src, dst = ext.at[e], uext.at[e]

        def put(base, rows, edge):
            for k, v in enumerate(apply(src, base, rows, edge)):
                dst[pl.ds(pl.multiple_of(base + k * block, 8), rows), :] = v

        put(at(0, GHOST - 1, PAD), cy, xe[0])

        def step(x, carry):
            put(at(0, x + GHOST), pitch, roll(cp[...], back(x)))
            return carry
        lax.fori_loop(0, cx, step, 0, unroll=UNROLL)
        put(at(0, GHOST + cx, PAD), cy, xe[1])
        put(at(0, GHOST + cx), PAD, roll(cp[0:PAD], -2 * cx - 1))

    def again(e, x):
        return apply(uext.at[e], at(0, x + GHOST, PAD), cy, roll(uz[...], back(x)))

    def once(e, x):
        return apply(ext.at[e], at(0, x + GHOST, PAD), cy, roll(cp[PAD:], back(x)))

    def reduce_start(n, gathered):
        line = jnp.zeros((1, LANES), jnp.float32)
        for j, acc in enumerate(gathered):
            part = jnp.sum(acc, axis=0, keepdims=True)
            for s in range(sets):
                value = jnp.sum(jnp.where(low == (s == 0), part, 0.0), axis=1, keepdims=True)
                line = jnp.where(lanes(1) == 2 * s + j, value, line)
        red_out[n] = line
        red[n, rank] = line
        for offset in offsets:
            pltpu.make_async_remote_copy(
                src_ref=red_out.at[n], dst_ref=red.at[n, rank], send_sem=red_send.at[n],
                recv_sem=red_recv.at[n], device_id=device_at(offset), device_id_type=MESH).start()

    def spread(v, j):
        value = jnp.sum(jnp.where(lanes(1) == j, v, 0.0), axis=1, keepdims=True)
        return jnp.broadcast_to(value, (1, LANES))

    def reduce_end(n):
        many = red.at[n, pl.ds(0, total - 1)]
        pltpu.make_async_copy(many, many, red_recv.at[n]).wait()
        pltpu.make_async_copy(many, many, red_send.at[n]).wait()
        line = jnp.sum(red[n], axis=0)
        return [jnp.where(low, spread(line, j), spread(line, 2 + j)) for j in range(2)]

    def take(v, index):
        return jnp.take_along_axis(v, index, axis=1)

    lane = lanes(cy)
    apart = 2 * (lane % HALF) + lane // HALF
    together = lane // 2 + HALF * (lane % 2)

    def permute(ref, index, rows):
        def step(m, carry):
            here = pl.ds(pl.multiple_of(m * cy, 8), cy)
            ref[here, :] = take(ref[here, :], index)
            return carry
        lax.fori_loop(0, rows // cy, step, 0, unroll=2 * UNROLL)

    def split(ref, x):
        a, b = ref[0, plain(x), :], ref[1, plain(x), :]
        return jnp.where(low, a, roll(b, HALF)), jnp.where(low, roll(a, HALF), b)

    def join(even_z, odd_z):
        return jnp.where(low, even_z, roll(odd_z, HALF)), jnp.where(low, roll(even_z, HALF), odd_z)

    def keep(e, x, pair):
        for k in range(2):
            ext[e, inner(k, x), :] = pair[k]

    def load(e, ref):
        for s in range(sets):
            permute(ref.at[s], apart, lines)

        def body(x):
            pair = split(ref, x)
            keep(e, x, pair)
            return pair, ()
        return sweep(body, 2 if e in DEEP else 1)[0]

    def load_kap(x):
        value = 4.0 * jnp.exp(-2.0 * lr_ref[plain(x), :])
        kap[plain(x), :] = value
        a = value + 6.0
        b = roll(a, HALF)
        pair = jnp.where(low, a, b), jnp.where(low, b, a)
        keep(KAP, x, pair)
        return pair, ()

    upper = lines // 2

    def observe(s):
        cell = idx_ref[s]
        value = val_ref[s]
        top = value.astype(jnp.bfloat16).astype(jnp.float32)
        line = cell // cz
        key = line // upper * LANES + cell % cz
        col = lax.broadcasted_iota(jnp.int32, (2 * LANES, nobs), 0)
        half = col % LANES // HALF
        hit = key == col // LANES * LANES + 2 * (col % HALF) + (half if s == 0 else 1 - half)
        for n, part in enumerate((1.0, top, value - top)):
            cols[2 * LANES * n:2 * LANES * (n + 1)] = jnp.where(hit, part, 0.0).astype(jnp.bfloat16)
        short = line % upper

        def step(m, carry):
            ids = lax.broadcasted_iota(jnp.int32, (upper, nobs), 0) + m * upper
            hot = jnp.where(ids == short, 1.0, 0.0).astype(jnp.bfloat16)
            got = lax.dot_general(hot, cols[...], (((1,), (1,)), ((), ())), preferred_element_type=jnp.float32)
            count = got[:, :2 * LANES] * (1.0 / noise_var)
            amount = (got[:, 2 * LANES:4 * LANES] + got[:, 4 * LANES:]) * (1.0 / noise_var)
            for h in range(2):
                here = pl.ds(pl.multiple_of(m * upper + h * upper, upper), upper)
                raw[s, 0, here, :] = count[:, h * LANES:(h + 1) * LANES]
                raw[s, 1, here, :] = amount[:, h * LANES:(h + 1) * LANES]
            return carry

        lax.fori_loop(0, 1, step, 0)

    loads[0].wait()
    faces_start = load(X0, start_ref)
    loads[3].wait()
    permute(lr_ref, apart, lines)
    faces_kap = sweep(load_kap, 1)[0]
    pl.semaphore_wait(barrier, total - 1)
    send_x(X0)
    send(X0, faces_start)
    send_x(KAP)
    send(KAP, faces_kap)
    loads[4].wait()
    faces_state = load(STATE, state_ref)
    send_x(STATE)
    send(STATE, faces_state)
    loads[1].wait()
    loads[2].wait()
    observe(0)
    observe(1)

    def mix(n, x):
        a, b = raw[0, n, plain(x), :], raw[1, n, plain(x), :]
        return jnp.where(low, a, b), roll(jnp.where(low, b, a), HALF)

    def right_pass(x):
        count, amount = mix(0, x), mix(1, x)
        for k in range(2):
            weight[dense(k, x), :] = count[k]
            rhs[dense(k, x), :] = amount[k] - count[k] * (ext[STATE, inner(k, x), :] + ext[X0, inner(k, x), :])
        return (None, None), ()

    sweep(right_pass)
    arrive(KAP)
    kz[...] = cp[PAD:]
    arrive(X0)
    wide(X0)

    def residual_pass(x):
        out = again(X0, x)
        pair = [rhs[dense(k, x), :] - out[k] for k in range(2)]
        keep(R0, x, pair)
        return pair, ()

    send(R0, sweep(residual_pass, 2, early=R0)[0])

    arrive(STATE)

    def state_pass(x):
        out = once(STATE, x)
        for k in range(2):
            ast[dense(k, x), :] = out[k]
        return (None, None), ()

    sweep(state_pass)

    arrive(R0)
    wide(R0)

    def image_pass(x):
        out = again(R0, x)
        now = [ext[R0, inner(k, x), :] for k in range(2)]
        pair = [out[k] + weight[dense(k, x), :] * now[k] for k in range(2)]
        keep(W0, x, pair)
        return pair, (now[0] * now[0] + now[1] * now[1], now[0] * pair[0] + now[1] * pair[1])

    faces, gathered = sweep(image_pass, 2, 2, early=W0)
    send(W0, faces)
    reduce_start(0, gathered)

    norms, steps, ratios = [], [], []
    for k, e in enumerate((W0, W1)):
        arrive(e)
        wide(e)

        def next_image(x, e=e):
            out = again(e, x)
            for p in range(2):
                q[dense(p, x), :] = out[p] + weight[dense(p, x), :] * ext[e, inner(p, x), :]
            return (None, None), ()

        sweep(next_image)
        norm, product = reduce_end(k)
        if k == 0:
            ratio, step_size = None, norm / product
        else:
            ratio = norm / norms[-1]
            step_size = norm / (product - ratio * norm / steps[-1])
        norms.append(norm)
        steps.append(step_size)
        ratios.append(ratio)

        def update(x, k=k, e=e, ratio=ratio, step_size=step_size):
            pair, terms = [], []
            for p in range(2):
                here, there = dense(p, x), inner(p, x)
                image, vec = q[here, :], ext[e, there, :]
                if k == 0:
                    z[here, :] = image
                    follow, now = vec, ext[R0, there, :]
                else:
                    image = image + ratio * z[here, :]
                    follow, now = vec + ratio * ext[W0, there, :], r[k - 1, here, :]
                    s_buf[here, :] = follow
                vec = vec - step_size * image
                now = now - step_size * follow
                ext[e + 1, there, :] = vec
                r[k, here, :] = now
                pair.append(vec)
                terms.append((now * now, now * vec))
            return pair, (terms[0][0] + terms[1][0], terms[0][1] + terms[1][1])

        faces, gathered = sweep(update, 2 if e + 1 in DEEP else 1, 2, early=e + 1)
        send(e + 1, faces)
        reduce_start(k + 1, gathered)

        def trail(x, k=k, ratio=ratio, step_size=step_size):
            for p in range(2):
                here, there = dense(p, x), inner(p, x)
                if k == 0:
                    xs[here, :] = ext[X0, there, :] + step_size * ext[R0, there, :]
                    now = uext[R0, there, :]
                    axs[here, :] = uext[X0, there, :] + step_size * now
                    ar[0, here, :] = now - step_size * uext[W0, there, :]
                else:
                    toward = r[0, here, :] + ratio * ext[R0, there, :]
                    rhs[here, :] = toward
                    xs[here, :] = xs[here, :] + step_size * toward
                    now = ar[0, here, :]
                    toward = now + ratio * uext[R0, there, :]
                    ad[here, :] = toward
                    axs[here, :] = axs[here, :] + step_size * toward
                    follow = uext[W1, there, :] + ratio * uext[W0, there, :]
                    q[here, :] = follow
                    ar[1, here, :] = now - step_size * follow
            return (None, None), ()

        sweep(trail)

    arrive(W2)

    def last_half(x):
        out = once(W2, x)
        for p in range(2):
            z[dense(p, x), :] = out[p]
        return (None, None), ()

    sweep(last_half)
    norm, product = reduce_end(2)
    ratio = norm / norms[-1]
    step_size = norm / (product - ratio * norm / steps[-1])

    def last_residual(x):
        norm_terms, terms = [], []
        for p in range(2):
            here, there = dense(p, x), inner(p, x)
            now = r[1, here, :] - step_size * (ext[W2, there, :] + ratio * s_buf[here, :])
            inner_now = ar[1, here, :] - step_size * (z[here, :] + ratio * q[here, :])
            r[2, here, :] = now
            ar[2, here, :] = inner_now
            norm_terms.append(now * now)
            terms.append(inner_now * inner_now + weight[here, :] * now * now)
        return (None, None), (norm_terms[0] + norm_terms[1], terms[0] + terms[1])

    reduce_start(3, sweep(last_residual, 0, 2)[1])

    def prepare(x):
        towards, olds, nows, grads = [], [], [], []
        for p in range(2):
            here, there = dense(p, x), inner(p, x)
            field, image = ext[STATE, there, :], ast[here, :]
            toward = r[1, here, :] + ratio * rhs[here, :]
            applied = ar[1, here, :] + ratio * ad[here, :]
            old = xs[here, :] + step_size * toward
            old_applied = axs[here, :] + step_size * applied
            now, now_applied = r[2, here, :], ar[2, here, :]
            towards.append(toward)
            olds.append(old)
            nows.append(now)
            grads.append((
                old * image + old_applied * field,
                now * image + now_applied * field,
                toward * image + applied * field,
            ))
        here = plain(x)
        scale = -2.0 * kap[here, :]
        for s, v in enumerate(join(*olds)):
            adj_ref[s, here, :] = v
        for n, pair in enumerate((nows, towards)):
            for s, v in enumerate(join(*pair)):
                raw[s, n, here, :] = v
        parts = [join(grads[0][n], grads[1][n]) for n in range(3)]
        grad_ref[here, :] = scale * (parts[0][0] + parts[0][1])
        for s in range(sets):
            gr[s, here, :] = scale * parts[1][s]
            gd[s, here, :] = scale * parts[2][s]
        return (None, None), ()

    sweep(prepare, unroll=4)
    for s in range(sets):
        permute(adj_ref.at[s], together, lines)
        for n in range(2):
            permute(raw.at[s, n], together, lines)
        permute(gr.at[s], together, lines)
        permute(gd.at[s], together, lines)
    permute(grad_ref, together, lines)
    last_norm, last_product = reduce_end(3)
    last_ratio = last_norm / norm
    last_step = last_norm / (last_product - last_ratio * last_norm / step_size)
    last_both = last_step * last_ratio
    one = [spread(last_step, s * HALF) for s in range(sets)]
    two = [spread(last_both, s * HALF) for s in range(sets)]

    def finish(x, carry):
        here = plain(x)
        grad = grad_ref[here, :]
        for s in range(sets):
            adj_ref[s, here, :] = adj_ref[s, here, :] + (one[s] * raw[s, 0, here, :] + two[s] * raw[s, 1, here, :])
            grad = grad + (one[s] * gr[s, here, :] + two[s] * gd[s, here, :])
        grad_ref[here, :] = grad
        return carry
    lax.fori_loop(0, cx, finish, 0, unroll=UNROLL)


def on_device(sizes, log_range, state, adjoint_start, obs_index, obs_value):
    sets, cx, cy, cz = state.shape
    nobs = obs_index.shape[-1]
    rows = cx * cy
    total = sizes[0] * sizes[1] * sizes[2]
    whole = 2 * (cx + 2 * GHOST) * (cy + PAD) + 8
    f32 = jnp.float32
    field = pltpu.VMEM((2 * rows, LANES), f32)
    natural = pltpu.VMEM((sets, rows, cz), f32)
    vmem = pl.BlockSpec(memory_space=pltpu.VMEM)
    gradient, adjoint = pl.pallas_call(
        functools.partial(kernel, sizes, (sets, cx, cy, cz, nobs)),
        out_shape=(
            jax.ShapeDtypeStruct((rows, cz), jnp.float32),
            jax.ShapeDtypeStruct((sets, rows, cz), jnp.float32),
        ),
        in_specs=[pl.BlockSpec(memory_space=pltpu.HBM)] * 5,
        out_specs=(vmem, vmem),
        scratch_shapes=[
            pltpu.VMEM((rows, cz), f32),
            natural,
            natural,
            pltpu.VMEM((sets, 1, nobs), jnp.int32),
            pltpu.VMEM((sets, 1, nobs), f32),
            pltpu.VMEM((FIELDS, whole, LANES), f32),
            pltpu.VMEM((len(DEEP), whole, LANES), f32),
            pltpu.VMEM((FIELDS, 2, GHOST, 2 * cx, LANES), f32),
            pltpu.VMEM((FIELDS, 2, GHOST, 2 * cx, LANES), f32),
            pltpu.VMEM((FIELDS, 2, cy, LANES), f32),
            pltpu.VMEM((FIELDS, 2, cy + 2 * PAD, LANES), f32),
            pltpu.VMEM((FIELDS, cy, LANES), f32),
            *[pltpu.VMEM((len(DEEP), 4, 8, LANES), f32)] * 4,
            pltpu.VMEM((cy + 2 * PAD, LANES), f32),
            pltpu.VMEM((cy + PAD, LANES), f32),
            pltpu.VMEM((2, cy, LANES), f32),
            pltpu.VMEM((cy, LANES), f32),
            pltpu.VMEM((cy, LANES), f32),
            pltpu.VMEM((rows, cz), f32),
            pltpu.VMEM((6 * LANES, nobs), jnp.bfloat16),
            pltpu.VMEM((sets, 2, rows, LANES), f32),
            field, field, field, field,
            pltpu.VMEM((3, 2 * rows, LANES), f32),
            pltpu.VMEM((3, 2 * rows, LANES), f32),
            *[field] * 5,
            natural, natural,
            pltpu.VMEM((ITERS, 1, LANES), f32),
            pltpu.VMEM((ITERS, total, 1, LANES), f32),
            pltpu.SemaphoreType.DMA((FIELDS, COPIES)),
            pltpu.SemaphoreType.DMA((FIELDS, COPIES)),
            pltpu.SemaphoreType.DMA((ITERS,)),
            pltpu.SemaphoreType.DMA((ITERS,)),
            pltpu.SemaphoreType.DMA((5,)),
        ],
        compiler_params=pltpu.CompilerParams(
            collective_id=0, has_side_effects=True, vmem_limit_bytes=63 * 1024 * 1024
        ),
    )(
        log_range.reshape(rows, cz),
        state.reshape(sets, rows, cz),
        adjoint_start.reshape(sets, rows, cz),
        obs_index.reshape(sets, 1, nobs),
        obs_value.reshape(sets, 1, nobs),
    )
    return gradient.reshape(cx, cy, cz), adjoint.reshape(sets, cx, cy, cz)


def solution(mesh):
    in_specs = (
        P("gx", "gy", "gz"),
        P(None, "gx", "gy", "gz"),
        P(None, "gx", "gy", "gz"),
        P(None, "gx", "gy", "gz", None),
        P(None, "gx", "gy", "gz", None),
    )
    out_specs = (P("gx", "gy", "gz"), P(None, "gx", "gy", "gz"))
    sizes = tuple(mesh.shape[axis] for axis in AXES)
    return jax.shard_map(
        functools.partial(on_device, sizes), mesh=mesh, in_specs=in_specs, out_specs=out_specs, check_vma=False
    )
```

```python
import functools
import itertools

import jax
import jax.numpy as jnp
from jax import lax
from jax.experimental import pallas as pl
from jax.experimental.pallas import tpu as pltpu
from jax.sharding import PartitionSpec as P

ITERS = 4
LANES = 128
HALF = LANES // 2
GHOST = 2
PAD = 8
AXES = ("gx", "gy", "gz")
MESH = pl.DeviceIdType.MESH
UNROLL = 8
X0, R0, W0, W1, W2, STATE, KAP, FIELDS = range(8)
DEEP = (X0, R0, W0, W1)
COPIES = 24

noise_var = 0.25


def kernel(
    sizes, dims, lr_hbm, state_hbm, start_hbm, idx_hbm, val_hbm, grad_ref, adj_ref,
    lr_ref, state_ref, start_ref, idx_ref, val_ref, ext, uext, ysend, yrecv, zsend, zrecv, zown, xysend, xyrecv, xzsend, xzrecv,
    ck, cp, xe, uz, kz, kap, cols, raw, weight, rhs, z, s_buf, r, ar, q, ast, ad, xs, axs,
    gr, gd, red_out, red, send_sem, recv_sem, red_send, red_recv, load_sem,
):
    sets, cx, cy, cz, nobs = dims
    pitch = cy + PAD
    slabs = cx + 2 * GHOST
    block = slabs * pitch
    lines = cx * cy
    groups = cy // 8
    place = [lax.axis_index(axis) for axis in AXES]
    rank = (place[0] * sizes[1] + place[1]) * sizes[2] + place[2]
    total = sizes[0] * sizes[1] * sizes[2]
    offsets = [o for o in itertools.product(*[range(n) for n in sizes]) if any(o)]

    def device_at(offset):
        return tuple(lax.rem(p + o % n, n) for p, o, n in zip(place, offset, sizes))

    barrier = pltpu.get_barrier_semaphore()
    for offset in offsets:
        pl.semaphore_signal(barrier, inc=1, device_id=device_at(offset), device_id_type=MESH)

    pairs = ((start_hbm, start_ref), (idx_hbm, idx_ref), (val_hbm, val_ref), (lr_hbm, lr_ref), (state_hbm, state_ref))
    loads = [pltpu.make_async_copy(a, b, load_sem.at[n]) for n, (a, b) in enumerate(pairs)]
    for copy in loads:
        copy.start()

    def lanes(rows):
        return lax.broadcasted_iota(jnp.int32, (rows, LANES), 1)

    def roll(v, n):
        n = n % LANES if isinstance(n, int) else n
        return v if isinstance(n, int) and n == 0 else pltpu.roll(v, n, 1)

    def back(x):
        return -2 * x - 1 if isinstance(x, int) else lax.rem(2 * LANES - 2 * x - 1, LANES)

    low = lanes(1) < HALF
    odd = lanes(1) % 2 == 1
    first = lanes(1) % HALF == 0
    end = lanes(1) % HALF == HALF - 1
    slot = lanes(cy) % HALF // 2

    def at(k, slab, row=0):
        return k * block + slab * pitch + row

    def inner(k, x):
        return pl.ds(pl.multiple_of(at(k, x + GHOST, PAD), 8), cy)

    def dense(k, x):
        return pl.ds(pl.multiple_of((k * cx + x) * cy, 8), cy)

    def plain(x):
        return pl.ds(pl.multiple_of(x * cy, 8), cy)

    def fold(v):
        return jnp.sum(v.reshape(groups, 8, LANES), axis=0)

    def sweep(body, pack=0, sums=0, unroll=UNROLL, early=None, after=None):
        zero = jnp.zeros((cy, LANES), jnp.float32)

        def step(x, carry):
            faces, gathered = carry
            (even_z, odd_z), terms = body(x)
            mixed = (jnp.where(first, even_z, odd_z), jnp.where(first, odd_z, even_z))[:pack] if pack else ()
            faces = tuple(jnp.where(slot == x, roll(m, 2 * x + 1), f) for m, f in zip(mixed, faces))
            return faces, tuple(a + fold(t) for a, t in zip(gathered, terms))

        start = (zero,) * pack, (jnp.zeros((8, LANES), jnp.float32),) * sums
        if early is None:
            return lax.fori_loop(0, cx, step, start, unroll=unroll)
        for x in (*range(GHOST), *range(cx - GHOST, cx)):
            start = step(x, start)
        send_x(early, start[0])
        far(after)
        return lax.fori_loop(GHOST, cx - GHOST, step, start, unroll=7)

    def copies(e):
        deep = e in DEEP
        out = []

        def add(offset, src, dst):
            n = len(out)
            out.append(pltpu.make_async_remote_copy(
                src_ref=src, dst_ref=dst, send_sem=send_sem.at[e, n], recv_sem=recv_sem.at[e, n],
                device_id=device_at(offset), device_id_type=MESH))

        corners = list(itertools.product((-1, 1), repeat=2)) if deep else []
        for n, (a, b) in enumerate(corners):
            add((a, 0, b), xzsend.at[e, n], xzrecv.at[e, n])
            add((a, b, 0), xysend.at[e, n], xyrecv.at[e, n])
        for k in range(2):
            for j in range(GHOST) if deep else (0,):
                add((-1, 0, 0), ext.at[e, pl.ds(at(k, GHOST + j, PAD), cy)],
                    ext.at[e, pl.ds(at(k, GHOST + cx + j, PAD), cy)])
                add((1, 0, 0), ext.at[e, pl.ds(at(k, GHOST + cx - 1 - j, PAD), cy)],
                    ext.at[e, pl.ds(at(k, GHOST - 1 - j, PAD), cy)])
        near = len(out)
        for a, b in corners:
            tile = slice(0, 8) if a < 0 else slice(cy - 8, cy)
            into = slice(PAD + cy, 2 * PAD + cy) if a < 0 else slice(0, PAD)
            add((0, a, b), zsend.at[e, (b + 1) // 2, tile], zrecv.at[e, (b + 1) // 2, into])
        add((0, 0, -1), zsend.at[e, 0], zrecv.at[e, 0, PAD:PAD + cy])
        add((0, 0, 1), zsend.at[e, 1], zrecv.at[e, 1, PAD:PAD + cy])
        planes = slice(0, GHOST if deep else 1)
        for side in range(2):
            add((0, 2 * side - 1, 0), ysend.at[e, side, planes], yrecv.at[e, side, planes])
        return out[:near], out[near:]

    def both_sides(faces):
        return jnp.where(odd, faces[0], roll(faces[1], -1)), jnp.where(odd, roll(faces[1], 1), faces[0])

    def send_x(e, faces=None):
        if e in DEEP:
            sides = both_sides(faces)
            for n, (a, b) in enumerate(itertools.product((-1, 1), repeat=2)):
                for k in range(2):
                    row = at(k, GHOST + (cx - 1 if a > 0 else 0), PAD + (cy - 1 if b > 0 else 0))
                    xysend[e, n, k:k + 1] = ext[e, row:row + 1, :]
                lane = (2 * (cx - 1) if a > 0 else 0) + (0 if b > 0 else 1)
                packed = jnp.zeros((8, LANES), jnp.float32)
                for g in range(groups):
                    part = roll(sides[(b + 1) // 2][8 * g:8 * g + 8], 2 * g)
                    packed = jnp.where(lanes(8) % HALF == (lane + 2 * g) % HALF, part, packed)
                xzsend[e, n] = packed
        for copy in copies(e)[0]:
            copy.start()

    def send(e, faces):
        zown[e] = faces[0]
        if e in DEEP:
            zsend[e, 0], zsend[e, 1] = both_sides(faces)
        else:
            zsend[e, 0] = faces[0]
            zsend[e, 1] = faces[0]
        for side in range(2):
            for plane in range(GHOST if e in DEEP else 1):
                y = cy - 1 - plane if side else plane
                for k in range(2):
                    ysend[e, side, plane, k * cx:(k + 1) * cx] = ext[e, pl.ds(at(k, GHOST, PAD + y), cx, stride=pitch), :]
        for copy in copies(e)[1]:
            copy.start()

    def arrive(e):
        faces, others = copies(e)
        planes = GHOST if e in DEEP else 1
        for copy in faces + others[-2:]:
            copy.wait()
        for side in range(2):
            for plane in range(planes):
                for k in range(2):
                    row = at(k, GHOST, PAD - 1 - plane if side else pitch + plane)
                    ext[e, pl.ds(row, cx, stride=pitch), :] = yrecv[e, side, plane, k * cx:(k + 1) * cx]
        if e in DEEP:
            side_x = [[None, None], [None, None]]
            for n, (a, b) in enumerate(itertools.product((-1, 1), repeat=2)):
                for k in range(2):
                    row = at(k, GHOST - 1 if a > 0 else GHOST + cx, PAD - 1 if b > 0 else pitch)
                    ext[e, row:row + 1, :] = xyrecv[e, n, k:k + 1]
                lane = (2 * (cx - 1) if a > 0 else 0) + (0 if b > 0 else 1)
                shift = -(lane + HALF) if b > 0 else HALF - 1 - lane
                side_x[0 if a > 0 else 1][0 if b > 0 else 1] = [
                    roll(xzrecv[e, n], shift - 2 * g) for g in range(groups)]
            for side in range(2):
                for g in range(groups):
                    xe[side, 8 * g:8 * g + 8] = jnp.where(first, side_x[side][0][g], side_x[side][1][g])
            pos = lanes(1) % HALF
            left_x, right_x = roll(xe[0], 1), roll(xe[1], 2 * cx - 1)
            uz[...] = zown[e] + jnp.where(pos < 2, left_x, 0.0) + jnp.where((pos >= 2 * cx - 2) & (pos < 2 * cx), right_x, 0.0)
        for copy in others[:-2]:
            copy.wait()
        if e not in DEEP:
            left, right = zrecv[e, 1, PAD:PAD + cy], zrecv[e, 0, PAD:PAD + cy]
            cp[PAD:] = jnp.where(odd, roll(left, HALF + 1), roll(right, HALF - 1))
            return
        left, right = zrecv[e, 1], zrecv[e, 0]
        both = jnp.where(odd, roll(left, HALF + 1), roll(right, HALF - 1))
        ck[...] = both
        beyond = roll(jnp.where(odd, left[PAD:PAD + cy], right[PAD:PAD + cy]), HALF)
        mid = both[PAD:PAD + cy]
        cp[PAD:] = mid
        top = lax.broadcasted_iota(jnp.int32, (PAD, LANES), 0) == 0
        cp[0:PAD] = jnp.where(top, roll(both[PAD + cy:], 2), both[0:PAD])
        around = uz[...] + beyond
        around = around + jnp.where(pos < 2, 0.0, roll(mid, 2))
        around = around + jnp.where((pos >= 2 * cx - 2) & (pos < 2 * cx), 0.0, roll(mid, -2))
        around = around + (ck[PAD - 1:PAD + cy - 1] + ck[PAD + 1:PAD + cy + 1])
        uz[...] = kz[...] * mid - around

    def apply(src, base, rows, edge):
        bases = [pl.multiple_of(base + k * block, 8) for k in range(2)]
        center = [src[pl.ds(b, rows), :] for b in bases]
        beside = [
            center[1] + jnp.where(first, edge, roll(center[1], 1)),
            center[0] + jnp.where(end, edge, roll(center[0], -1)),
        ]
        out = []
        for k, b in enumerate(bases):
            around = src[pl.ds(b + pitch, rows), :] + src[pl.ds(b - pitch, rows), :]
            around = around + (src[pl.ds(b + 1, rows), :] + src[pl.ds(b - 1, rows), :])
            out.append(ext[KAP, pl.ds(b, rows), :] * center[k] - (around + beside[k]))
        return out

    def put(e, base, rows, edge):
        for k, v in enumerate(apply(ext.at[e], base, rows, edge)):
            uext[e, pl.ds(pl.multiple_of(base + k * block, 8), rows), :] = v

    def wide(e, x):
        put(e, at(0, x + GHOST), pitch, roll(cp[...], back(x)))

    def near(e):
        put(e, at(0, GHOST - 1, PAD), cy, xe[0])
        for x in (*range(GHOST + 1), *range(cx - GHOST - 1, cx)):
            wide(e, x)
        put(e, at(0, GHOST + cx, PAD), cy, xe[1])
        put(e, at(0, GHOST + cx), PAD, roll(cp[0:PAD], -2 * cx - 1))

    def far(e):
        def step(x, carry):
            wide(e, x)
            return carry
        lax.fori_loop(GHOST + 1, cx - GHOST - 1, step, 0, unroll=13)

    def again(e, x):
        return apply(uext.at[e], at(0, x + GHOST, PAD), cy, roll(uz[...], back(x)))

    def once(e, x):
        return apply(ext.at[e], at(0, x + GHOST, PAD), cy, roll(cp[PAD:], back(x)))

    def reduce_start(n, gathered):
        line = jnp.zeros((1, LANES), jnp.float32)
        for j, acc in enumerate(gathered):
            part = jnp.sum(acc, axis=0, keepdims=True)
            for s in range(sets):
                value = jnp.sum(jnp.where(low == (s == 0), part, 0.0), axis=1, keepdims=True)
                line = jnp.where(lanes(1) == 2 * s + j, value, line)
        red_out[n] = line
        red[n, rank] = line
        for offset in offsets:
            pltpu.make_async_remote_copy(
                src_ref=red_out.at[n], dst_ref=red.at[n, rank], send_sem=red_send.at[n],
                recv_sem=red_recv.at[n], device_id=device_at(offset), device_id_type=MESH).start()

    def spread(v, j):
        value = jnp.sum(jnp.where(lanes(1) == j, v, 0.0), axis=1, keepdims=True)
        return jnp.broadcast_to(value, (1, LANES))

    def reduce_end(n):
        many = red.at[n, pl.ds(0, total - 1)]
        pltpu.make_async_copy(many, many, red_recv.at[n]).wait()
        pltpu.make_async_copy(many, many, red_send.at[n]).wait()
        line = jnp.sum(red[n], axis=0)
        return [jnp.where(low, spread(line, j), spread(line, 2 + j)) for j in range(2)]

    def take(v, index):
        return jnp.take_along_axis(v, index, axis=1)

    lane = lanes(cy)
    apart = [2 * (lane % HALF) + (lane // HALF if s == 0 else 1 - lane // HALF) for s in range(sets)]
    together = [lane // 2 + HALF * (lane % 2 if s == 0 else 1 - lane % 2) for s in range(sets)]

    def permute(ref, index, rows):
        def step(m, carry):
            here = pl.ds(pl.multiple_of(m * cy, 8), cy)
            ref[here, :] = take(ref[here, :], index)
            return carry
        lax.fori_loop(0, rows // cy, step, 0, unroll=2 * UNROLL)

    def split(ref, x):
        a, b = ref[0, plain(x), :], ref[1, plain(x), :]
        return jnp.where(low, a, b), roll(jnp.where(low, b, a), HALF)

    def join(even_z, odd_z):
        turned = roll(odd_z, HALF)
        return jnp.where(low, even_z, turned), jnp.where(low, turned, even_z)

    def keep(e, x, pair):
        for k in range(2):
            ext[e, inner(k, x), :] = pair[k]

    def load(e, ref):
        def body(x):
            pair = split(ref, x)
            keep(e, x, pair)
            return pair, ()
        return sweep(body, 2 if e in DEEP else 1)[0]

    def load_kap(x):
        value = 4.0 * jnp.exp(-2.0 * lr_ref[plain(x), :])
        kap[plain(x), :] = value
        a = value + 6.0
        b = roll(a, HALF)
        pair = jnp.where(low, a, b), jnp.where(low, b, a)
        keep(KAP, x, pair)
        return pair, ()

    upper = lines // 2

    def observe(s):
        cell = idx_ref[s]
        value = val_ref[s]
        top = value.astype(jnp.bfloat16).astype(jnp.float32)
        line = cell // cz
        key = line // upper * LANES + cell % cz
        col = lax.broadcasted_iota(jnp.int32, (2 * LANES, nobs), 0)
        half = col % LANES // HALF
        hit = key == col // LANES * LANES + 2 * (col % HALF) + (half if s == 0 else 1 - half)
        for n, part in enumerate((1.0, top, value - top)):
            cols[2 * LANES * n:2 * LANES * (n + 1)] = jnp.where(hit, part, 0.0).astype(jnp.bfloat16)
        short = line % upper

        def step(m, carry):
            ids = lax.broadcasted_iota(jnp.int32, (upper, nobs), 0) + m * upper
            hot = jnp.where(ids == short, 1.0, 0.0).astype(jnp.bfloat16)
            got = lax.dot_general(hot, cols[...], (((1,), (1,)), ((), ())), preferred_element_type=jnp.float32)
            count = got[:, :2 * LANES] * (1.0 / noise_var)
            amount = (got[:, 2 * LANES:4 * LANES] + got[:, 4 * LANES:]) * (1.0 / noise_var)
            for h in range(2):
                here = pl.ds(pl.multiple_of(m * upper + h * upper, upper), upper)
                raw[s, 0, here, :] = count[:, h * LANES:(h + 1) * LANES]
                raw[s, 1, here, :] = amount[:, h * LANES:(h + 1) * LANES]
            return carry

        lax.fori_loop(0, 1, step, 0)

    loads[0].wait()
    for s in range(sets):
        permute(start_ref.at[s], apart[s], lines)
    faces_start = load(X0, start_ref)
    loads[3].wait()
    permute(lr_ref, apart[0], lines)
    faces_kap = sweep(load_kap, 1)[0]
    pl.semaphore_wait(barrier, total - 1)
    send_x(X0, faces_start)
    send(X0, faces_start)
    send_x(KAP)
    send(KAP, faces_kap)
    loads[4].wait()
    for s in range(sets):
        permute(state_ref.at[s], apart[s], lines)
    loads[1].wait()
    loads[2].wait()
    observe(0)
    observe(1)

    def right_pass(x):
        here = plain(x)
        counts = [raw[s, 0, here, :] for s in range(sets)]
        right = [raw[s, 1, here, :] - counts[s] * (state_ref[s, here, :] + start_ref[s, here, :]) for s in range(sets)]
        for ref, (a, b) in ((weight, counts), (rhs, right)):
            ref[dense(0, x), :] = jnp.where(low, a, b)
            ref[dense(1, x), :] = roll(jnp.where(low, b, a), HALF)
        return (None, None), ()

    sweep(right_pass)
    arrive(KAP)
    kz[...] = cp[PAD:]
    arrive(X0)
    near(X0)

    def residual_pass(x):
        out = again(X0, x)
        pair = [rhs[dense(k, x), :] - out[k] for k in range(2)]
        keep(R0, x, pair)
        return pair, ()

    send(R0, sweep(residual_pass, 2, early=R0, after=X0)[0])

    faces = load(STATE, state_ref)
    send_x(STATE)
    send(STATE, faces)

    arrive(R0)
    near(R0)

    def image_pass(x):
        out = again(R0, x)
        now = [ext[R0, inner(k, x), :] for k in range(2)]
        pair = [out[k] + weight[dense(k, x), :] * now[k] for k in range(2)]
        keep(W0, x, pair)
        return pair, (now[0] * now[0] + now[1] * now[1], now[0] * pair[0] + now[1] * pair[1])

    faces, gathered = sweep(image_pass, 2, 2, early=W0, after=R0)
    reduce_start(0, gathered)
    send(W0, faces)

    arrive(STATE)

    def state_pass(x):
        out = once(STATE, x)
        for k in range(2):
            ast[dense(k, x), :] = out[k]
        return (None, None), ()

    sweep(state_pass)

    norms, steps, ratios = [], [], []
    for k, e in enumerate((W0, W1)):
        arrive(e)
        near(e)
        norm, product = reduce_end(k)
        if k == 0:
            ratio, step_size = None, norm / product
        else:
            ratio = norm / norms[-1]
            step_size = norm / (product - ratio * norm / steps[-1])
        norms.append(norm)
        steps.append(step_size)
        ratios.append(ratio)

        def update(x, k=k, e=e, ratio=ratio, step_size=step_size):
            pair, terms, out = [], [], again(e, x)
            for p in range(2):
                here, there = dense(p, x), inner(p, x)
                vec = ext[e, there, :]
                image = out[p] + weight[here, :] * vec
                if k == 0:
                    z[here, :] = image
                    follow, now = vec, ext[R0, there, :]
                else:
                    image = image + ratio * z[here, :]
                    follow, now = vec + ratio * ext[W0, there, :], r[k - 1, here, :]
                    s_buf[here, :] = follow
                vec = vec - step_size * image
                now = now - step_size * follow
                ext[e + 1, there, :] = vec
                r[k, here, :] = now
                pair.append(vec)
                terms.append((now * now, now * vec))
            return pair, (terms[0][0] + terms[1][0], terms[0][1] + terms[1][1])

        faces, gathered = sweep(update, 2 if e + 1 in DEEP else 1, 2, early=e + 1, after=e)
        reduce_start(k + 1, gathered)
        send(e + 1, faces)

        def trail(x, k=k, ratio=ratio, step_size=step_size):
            for p in range(2):
                here, there = dense(p, x), inner(p, x)
                if k == 0:
                    xs[here, :] = ext[X0, there, :] + step_size * ext[R0, there, :]
                    now = uext[R0, there, :]
                    axs[here, :] = uext[X0, there, :] + step_size * now
                    ar[0, here, :] = now - step_size * uext[W0, there, :]
                else:
                    toward = r[0, here, :] + ratio * ext[R0, there, :]
                    rhs[here, :] = toward
                    xs[here, :] = xs[here, :] + step_size * toward
                    now = ar[0, here, :]
                    toward = now + ratio * uext[R0, there, :]
                    ad[here, :] = toward
                    axs[here, :] = axs[here, :] + step_size * toward
                    follow = uext[W1, there, :] + ratio * uext[W0, there, :]
                    q[here, :] = follow
                    ar[1, here, :] = now - step_size * follow
            return (None, None), ()

        sweep(trail)

    arrive(W2)

    def last_half(x):
        out = once(W2, x)
        for p in range(2):
            z[dense(p, x), :] = out[p]
        return (None, None), ()

    sweep(last_half)
    norm, product = reduce_end(2)
    ratio = norm / norms[-1]
    step_size = norm / (product - ratio * norm / steps[-1])

    def last_residual(x):
        norm_terms, terms = [], []
        for p in range(2):
            here, there = dense(p, x), inner(p, x)
            now = r[1, here, :] - step_size * (ext[W2, there, :] + ratio * s_buf[here, :])
            inner_now = ar[1, here, :] - step_size * (z[here, :] + ratio * q[here, :])
            r[2, here, :] = now
            ar[2, here, :] = inner_now
            norm_terms.append(now * now)
            terms.append(inner_now * inner_now + weight[here, :] * now * now)
        return (None, None), (norm_terms[0] + norm_terms[1], terms[0] + terms[1])

    reduce_start(3, sweep(last_residual, 0, 2)[1])

    def prepare(x):
        towards, olds, nows, grads = [], [], [], []
        for p in range(2):
            here, there = dense(p, x), inner(p, x)
            field, image = ext[STATE, there, :], ast[here, :]
            toward = r[1, here, :] + ratio * rhs[here, :]
            applied = ar[1, here, :] + ratio * ad[here, :]
            old = xs[here, :] + step_size * toward
            old_applied = axs[here, :] + step_size * applied
            now, now_applied = r[2, here, :], ar[2, here, :]
            towards.append(toward)
            olds.append(old)
            nows.append(now)
            grads.append((
                old * image + old_applied * field,
                now * image + now_applied * field,
                toward * image + applied * field,
            ))
        here = plain(x)
        scale = -2.0 * kap[here, :]
        for s, v in enumerate(join(*olds)):
            adj_ref[s, here, :] = v
        for n, pair in enumerate((nows, towards)):
            for s, v in enumerate(join(*pair)):
                raw[s, n, here, :] = v
        parts = [join(grads[0][n], grads[1][n]) for n in range(3)]
        grad_ref[here, :] = scale * (parts[0][0] + roll(parts[0][1], HALF))
        for s, factor in enumerate((scale, roll(scale, HALF))):
            gr[s, here, :] = factor * parts[1][s]
            gd[s, here, :] = factor * parts[2][s]
        return (None, None), ()

    sweep(prepare, unroll=4)
    for s in range(sets):
        for ref in (adj_ref.at[s], raw.at[s, 0], raw.at[s, 1], gr.at[s], gd.at[s]):
            permute(ref, together[s], lines)
    permute(grad_ref, together[0], lines)
    last_norm, last_product = reduce_end(3)
    last_ratio = last_norm / norm
    last_step = last_norm / (last_product - last_ratio * last_norm / step_size)
    last_both = last_step * last_ratio
    one = [spread(last_step, s * HALF) for s in range(sets)]
    two = [spread(last_both, s * HALF) for s in range(sets)]

    def finish(x, carry):
        here = plain(x)
        grad = grad_ref[here, :]
        for s in range(sets):
            adj_ref[s, here, :] = adj_ref[s, here, :] + (one[s] * raw[s, 0, here, :] + two[s] * raw[s, 1, here, :])
            grad = grad + (one[s] * gr[s, here, :] + two[s] * gd[s, here, :])
        grad_ref[here, :] = grad
        return carry
    lax.fori_loop(0, cx, finish, 0, unroll=UNROLL)


def on_device(sizes, log_range, state, adjoint_start, obs_index, obs_value):
    sets, cx, cy, cz = state.shape
    nobs = obs_index.shape[-1]
    rows = cx * cy
    total = sizes[0] * sizes[1] * sizes[2]
    whole = 2 * (cx + 2 * GHOST) * (cy + PAD) + 8
    f32 = jnp.float32
    field = pltpu.VMEM((2 * rows, LANES), f32)
    natural = pltpu.VMEM((sets, rows, cz), f32)
    vmem = pl.BlockSpec(memory_space=pltpu.VMEM)
    gradient, adjoint = pl.pallas_call(
        functools.partial(kernel, sizes, (sets, cx, cy, cz, nobs)),
        out_shape=(
            jax.ShapeDtypeStruct((rows, cz), jnp.float32),
            jax.ShapeDtypeStruct((sets, rows, cz), jnp.float32),
        ),
        in_specs=[pl.BlockSpec(memory_space=pltpu.HBM)] * 5,
        out_specs=(vmem, vmem),
        scratch_shapes=[
            pltpu.VMEM((rows, cz), f32),
            natural,
            natural,
            pltpu.VMEM((sets, 1, nobs), jnp.int32),
            pltpu.VMEM((sets, 1, nobs), f32),
            pltpu.VMEM((FIELDS, whole, LANES), f32),
            pltpu.VMEM((len(DEEP), whole, LANES), f32),
            pltpu.VMEM((FIELDS, 2, GHOST, 2 * cx, LANES), f32),
            pltpu.VMEM((FIELDS, 2, GHOST, 2 * cx, LANES), f32),
            pltpu.VMEM((FIELDS, 2, cy, LANES), f32),
            pltpu.VMEM((FIELDS, 2, cy + 2 * PAD, LANES), f32),
            pltpu.VMEM((FIELDS, cy, LANES), f32),
            *[pltpu.VMEM((len(DEEP), 4, 8, LANES), f32)] * 4,
            pltpu.VMEM((cy + 2 * PAD, LANES), f32),
            pltpu.VMEM((cy + PAD, LANES), f32),
            pltpu.VMEM((2, cy, LANES), f32),
            pltpu.VMEM((cy, LANES), f32),
            pltpu.VMEM((cy, LANES), f32),
            pltpu.VMEM((rows, cz), f32),
            pltpu.VMEM((6 * LANES, nobs), jnp.bfloat16),
            pltpu.VMEM((sets, 2, rows, LANES), f32),
            field, field, field, field,
            pltpu.VMEM((3, 2 * rows, LANES), f32),
            pltpu.VMEM((3, 2 * rows, LANES), f32),
            *[field] * 5,
            natural, natural,
            pltpu.VMEM((ITERS, 1, LANES), f32),
            pltpu.VMEM((ITERS, total, 1, LANES), f32),
            pltpu.SemaphoreType.DMA((FIELDS, COPIES)),
            pltpu.SemaphoreType.DMA((FIELDS, COPIES)),
            pltpu.SemaphoreType.DMA((ITERS,)),
            pltpu.SemaphoreType.DMA((ITERS,)),
            pltpu.SemaphoreType.DMA((5,)),
        ],
        compiler_params=pltpu.CompilerParams(
            collective_id=0, has_side_effects=True, vmem_limit_bytes=63 * 1024 * 1024
        ),
    )(
        log_range.reshape(rows, cz),
        state.reshape(sets, rows, cz),
        adjoint_start.reshape(sets, rows, cz),
        obs_index.reshape(sets, 1, nobs),
        obs_value.reshape(sets, 1, nobs),
    )
    return gradient.reshape(cx, cy, cz), adjoint.reshape(sets, cx, cy, cz)


def solution(mesh):
    in_specs = (
        P("gx", "gy", "gz"),
        P(None, "gx", "gy", "gz"),
        P(None, "gx", "gy", "gz"),
        P(None, "gx", "gy", "gz", None),
        P(None, "gx", "gy", "gz", None),
    )
    out_specs = (P("gx", "gy", "gz"), P(None, "gx", "gy", "gz"))
    sizes = tuple(mesh.shape[axis] for axis in AXES)
    return jax.shard_map(
        functools.partial(on_device, sizes), mesh=mesh, in_specs=in_specs, out_specs=out_specs, check_vma=False
    )
```

```python
import functools
import itertools

import jax
import jax.numpy as jnp
from jax import lax
from jax.experimental import pallas as pl
from jax.experimental.pallas import tpu as pltpu
from jax.sharding import PartitionSpec as P

ITERS = 4
LANES = 128
HALF = LANES // 2
GHOST = 2
PAD = 8
AXES = ("gx", "gy", "gz")
MESH = pl.DeviceIdType.MESH
UNROLL = 8
CHUNKS = 4
X0, R0, W0, W1, W2, STATE, KAP, FIELDS = range(8)
DEEP = (X0, R0, W0, W1)
COPIES = 24

noise_var = 0.25


def kernel(
    sizes, dims, lr_hbm, state_hbm, start_hbm, idx_hbm, val_hbm, grad_hbm, adj_hbm,
    grad_ref, adj_ref, lr_ref, state_ref, start_ref, idx_ref, val_ref, ext, uext, ysend, yrecv, zsend, zrecv, zown, xysend, xyrecv, xzsend, xzrecv,
    ck, cp, xe, uz, kz, kap, cols, raw, weight, rhs, z, s_buf, r, ar, q, ast, ad, xs, axs,
    gr, gd, red_out, red, send_sem, recv_sem, red_send, red_recv, load_sem, store_sem,
):
    sets, cx, cy, cz, nobs = dims
    pitch = cy + PAD
    slabs = cx + 2 * GHOST
    block = slabs * pitch
    lines = cx * cy
    groups = cy // 8
    place = [lax.axis_index(axis) for axis in AXES]
    rank = (place[0] * sizes[1] + place[1]) * sizes[2] + place[2]
    total = sizes[0] * sizes[1] * sizes[2]
    offsets = [o for o in itertools.product(*[range(n) for n in sizes]) if any(o)]

    def device_at(offset):
        return tuple(lax.rem(p + o % n, n) for p, o, n in zip(place, offset, sizes))

    barrier = pltpu.get_barrier_semaphore()
    for offset in offsets:
        pl.semaphore_signal(barrier, inc=1, device_id=device_at(offset), device_id_type=MESH)

    pairs = ((start_hbm, start_ref), (idx_hbm, idx_ref), (val_hbm, val_ref), (lr_hbm, lr_ref), (state_hbm, state_ref))
    loads = [pltpu.make_async_copy(a, b, load_sem.at[n]) for n, (a, b) in enumerate(pairs)]
    for copy in loads:
        copy.start()

    def lanes(rows):
        return lax.broadcasted_iota(jnp.int32, (rows, LANES), 1)

    def roll(v, n):
        n = n % LANES if isinstance(n, int) else n
        return v if isinstance(n, int) and n == 0 else pltpu.roll(v, n, 1)

    def back(x):
        return -2 * x - 1 if isinstance(x, int) else lax.rem(2 * LANES - 2 * x - 1, LANES)

    low = lanes(1) < HALF
    odd = lanes(1) % 2 == 1
    first = lanes(1) % HALF == 0
    end = lanes(1) % HALF == HALF - 1
    slot = lanes(cy) % HALF // 2

    def at(k, slab, row=0):
        return k * block + slab * pitch + row

    def inner(k, x):
        return pl.ds(pl.multiple_of(at(k, x + GHOST, PAD), 8), cy)

    def dense(k, x):
        return pl.ds(pl.multiple_of((k * cx + x) * cy, 8), cy)

    def plain(x):
        return pl.ds(pl.multiple_of(x * cy, 8), cy)

    def fold(v):
        return jnp.sum(v.reshape(groups, 8, LANES), axis=0)

    def sweep(body, pack=0, sums=0, unroll=UNROLL, early=None, after=None):
        zero = jnp.zeros((cy, LANES), jnp.float32)

        def step(x, carry):
            faces, gathered = carry
            (even_z, odd_z), terms = body(x)
            mixed = (jnp.where(first, even_z, odd_z), jnp.where(first, odd_z, even_z))[:pack] if pack else ()
            faces = tuple(jnp.where(slot == x, roll(m, 2 * x + 1), f) for m, f in zip(mixed, faces))
            return faces, tuple(a + fold(t) for a, t in zip(gathered, terms))

        start = (zero,) * pack, (jnp.zeros((8, LANES), jnp.float32),) * sums
        if early is None:
            return lax.fori_loop(0, cx, step, start, unroll=unroll)
        for x in (*range(GHOST), *range(cx - GHOST, cx)):
            start = step(x, start)
        send_x(early, start[0])
        far(after)
        return lax.fori_loop(GHOST, cx - GHOST, step, start, unroll=7)

    def copies(e):
        deep = e in DEEP
        out = []

        def add(offset, src, dst):
            n = len(out)
            out.append(pltpu.make_async_remote_copy(
                src_ref=src, dst_ref=dst, send_sem=send_sem.at[e, n], recv_sem=recv_sem.at[e, n],
                device_id=device_at(offset), device_id_type=MESH))

        corners = list(itertools.product((-1, 1), repeat=2)) if deep else []
        for n, (a, b) in enumerate(corners):
            add((a, 0, b), xzsend.at[e, n], xzrecv.at[e, n])
            add((a, b, 0), xysend.at[e, n], xyrecv.at[e, n])
        for k in range(2):
            for j in range(GHOST) if deep else (0,):
                add((-1, 0, 0), ext.at[e, pl.ds(at(k, GHOST + j, PAD), cy)],
                    ext.at[e, pl.ds(at(k, GHOST + cx + j, PAD), cy)])
                add((1, 0, 0), ext.at[e, pl.ds(at(k, GHOST + cx - 1 - j, PAD), cy)],
                    ext.at[e, pl.ds(at(k, GHOST - 1 - j, PAD), cy)])
        near = len(out)
        for a, b in corners:
            tile = slice(0, 8) if a < 0 else slice(cy - 8, cy)
            into = slice(PAD + cy, 2 * PAD + cy) if a < 0 else slice(0, PAD)
            add((0, a, b), zsend.at[e, (b + 1) // 2, tile], zrecv.at[e, (b + 1) // 2, into])
        add((0, 0, -1), zsend.at[e, 0], zrecv.at[e, 0, PAD:PAD + cy])
        add((0, 0, 1), zsend.at[e, 1], zrecv.at[e, 1, PAD:PAD + cy])
        planes = slice(0, GHOST if deep else 1)
        for side in range(2):
            add((0, 2 * side - 1, 0), ysend.at[e, side, planes], yrecv.at[e, side, planes])
        return out[:near], out[near:]

    def both_sides(faces):
        return jnp.where(odd, faces[0], roll(faces[1], -1)), jnp.where(odd, roll(faces[1], 1), faces[0])

    def send_x(e, faces=None):
        if e in DEEP:
            sides = both_sides(faces)
            for n, (a, b) in enumerate(itertools.product((-1, 1), repeat=2)):
                for k in range(2):
                    row = at(k, GHOST + (cx - 1 if a > 0 else 0), PAD + (cy - 1 if b > 0 else 0))
                    xysend[e, n, k:k + 1] = ext[e, row:row + 1, :]
                lane = (2 * (cx - 1) if a > 0 else 0) + (0 if b > 0 else 1)
                packed = jnp.zeros((8, LANES), jnp.float32)
                for g in range(groups):
                    part = roll(sides[(b + 1) // 2][8 * g:8 * g + 8], 2 * g)
                    packed = jnp.where(lanes(8) % HALF == (lane + 2 * g) % HALF, part, packed)
                xzsend[e, n] = packed
        for copy in copies(e)[0]:
            copy.start()

    def send(e, faces):
        zown[e] = faces[0]
        if e in DEEP:
            zsend[e, 0], zsend[e, 1] = both_sides(faces)
        else:
            zsend[e, 0] = faces[0]
            zsend[e, 1] = faces[0]
        for side in range(2):
            for plane in range(GHOST if e in DEEP else 1):
                y = cy - 1 - plane if side else plane
                for k in range(2):
                    ysend[e, side, plane, k * cx:(k + 1) * cx] = ext[e, pl.ds(at(k, GHOST, PAD + y), cx, stride=pitch), :]
        for copy in copies(e)[1]:
            copy.start()

    def arrive(e):
        faces, others = copies(e)
        planes = GHOST if e in DEEP else 1
        for copy in faces + others[-2:]:
            copy.wait()
        for side in range(2):
            for plane in range(planes):
                for k in range(2):
                    row = at(k, GHOST, PAD - 1 - plane if side else pitch + plane)
                    ext[e, pl.ds(row, cx, stride=pitch), :] = yrecv[e, side, plane, k * cx:(k + 1) * cx]
        if e in DEEP:
            side_x = [[None, None], [None, None]]
            for n, (a, b) in enumerate(itertools.product((-1, 1), repeat=2)):
                for k in range(2):
                    row = at(k, GHOST - 1 if a > 0 else GHOST + cx, PAD - 1 if b > 0 else pitch)
                    ext[e, row:row + 1, :] = xyrecv[e, n, k:k + 1]
                lane = (2 * (cx - 1) if a > 0 else 0) + (0 if b > 0 else 1)
                shift = -(lane + HALF) if b > 0 else HALF - 1 - lane
                side_x[0 if a > 0 else 1][0 if b > 0 else 1] = [
                    roll(xzrecv[e, n], shift - 2 * g) for g in range(groups)]
            for side in range(2):
                for g in range(groups):
                    xe[side, 8 * g:8 * g + 8] = jnp.where(first, side_x[side][0][g], side_x[side][1][g])
            pos = lanes(1) % HALF
            left_x, right_x = roll(xe[0], 1), roll(xe[1], 2 * cx - 1)
            uz[...] = zown[e] + jnp.where(pos < 2, left_x, 0.0) + jnp.where((pos >= 2 * cx - 2) & (pos < 2 * cx), right_x, 0.0)
        for copy in others[:-2]:
            copy.wait()
        if e not in DEEP:
            left, right = zrecv[e, 1, PAD:PAD + cy], zrecv[e, 0, PAD:PAD + cy]
            cp[PAD:] = jnp.where(odd, roll(left, HALF + 1), roll(right, HALF - 1))
            return
        left, right = zrecv[e, 1], zrecv[e, 0]
        both = jnp.where(odd, roll(left, HALF + 1), roll(right, HALF - 1))
        ck[...] = both
        beyond = roll(jnp.where(odd, left[PAD:PAD + cy], right[PAD:PAD + cy]), HALF)
        mid = both[PAD:PAD + cy]
        cp[PAD:] = mid
        top = lax.broadcasted_iota(jnp.int32, (PAD, LANES), 0) == 0
        cp[0:PAD] = jnp.where(top, roll(both[PAD + cy:], 2), both[0:PAD])
        around = uz[...] + beyond
        around = around + jnp.where(pos < 2, 0.0, roll(mid, 2))
        around = around + jnp.where((pos >= 2 * cx - 2) & (pos < 2 * cx), 0.0, roll(mid, -2))
        around = around + (ck[PAD - 1:PAD + cy - 1] + ck[PAD + 1:PAD + cy + 1])
        uz[...] = kz[...] * mid - around

    def apply(src, base, rows, edge):
        bases = [pl.multiple_of(base + k * block, 8) for k in range(2)]
        center = [src[pl.ds(b, rows), :] for b in bases]
        beside = [
            center[1] + jnp.where(first, edge, roll(center[1], 1)),
            center[0] + jnp.where(end, edge, roll(center[0], -1)),
        ]
        out = []
        for k, b in enumerate(bases):
            around = src[pl.ds(b + pitch, rows), :] + src[pl.ds(b - pitch, rows), :]
            around = around + (src[pl.ds(b + 1, rows), :] + src[pl.ds(b - 1, rows), :])
            out.append(ext[KAP, pl.ds(b, rows), :] * center[k] - (around + beside[k]))
        return out

    def put(e, base, rows, edge):
        for k, v in enumerate(apply(ext.at[e], base, rows, edge)):
            uext[e, pl.ds(pl.multiple_of(base + k * block, 8), rows), :] = v

    def wide(e, x):
        put(e, at(0, x + GHOST), pitch, roll(cp[...], back(x)))

    def near(e):
        put(e, at(0, GHOST - 1, PAD), cy, xe[0])
        for x in (*range(GHOST + 1), *range(cx - GHOST - 1, cx)):
            wide(e, x)
        put(e, at(0, GHOST + cx, PAD), cy, xe[1])
        put(e, at(0, GHOST + cx), PAD, roll(cp[0:PAD], -2 * cx - 1))

    def far(e):
        def step(x, carry):
            wide(e, x)
            return carry
        lax.fori_loop(GHOST + 1, cx - GHOST - 1, step, 0, unroll=13)

    def again(e, x):
        return apply(uext.at[e], at(0, x + GHOST, PAD), cy, roll(uz[...], back(x)))

    def once(e, x):
        return apply(ext.at[e], at(0, x + GHOST, PAD), cy, roll(cp[PAD:], back(x)))

    def reduce_start(n, gathered):
        line = jnp.zeros((1, LANES), jnp.float32)
        for j, acc in enumerate(gathered):
            part = jnp.sum(acc, axis=0, keepdims=True)
            for s in range(sets):
                value = jnp.sum(jnp.where(low == (s == 0), part, 0.0), axis=1, keepdims=True)
                line = jnp.where(lanes(1) == 2 * s + j, value, line)
        red_out[n] = line
        red[n, rank] = line
        for offset in offsets:
            pltpu.make_async_remote_copy(
                src_ref=red_out.at[n], dst_ref=red.at[n, rank], send_sem=red_send.at[n],
                recv_sem=red_recv.at[n], device_id=device_at(offset), device_id_type=MESH).start()

    def spread(v, j):
        value = jnp.sum(jnp.where(lanes(1) == j, v, 0.0), axis=1, keepdims=True)
        return jnp.broadcast_to(value, (1, LANES))

    def reduce_end(n):
        many = red.at[n, pl.ds(0, total - 1)]
        pltpu.make_async_copy(many, many, red_recv.at[n]).wait()
        pltpu.make_async_copy(many, many, red_send.at[n]).wait()
        line = jnp.sum(red[n], axis=0)
        return [jnp.where(low, spread(line, j), spread(line, 2 + j)) for j in range(2)]

    def take(v, index):
        return jnp.take_along_axis(v, index, axis=1)

    lane = lanes(cy)
    apart = [2 * (lane % HALF) + (lane // HALF if s == 0 else 1 - lane // HALF) for s in range(sets)]
    together = [lane // 2 + HALF * (lane % 2 if s == 0 else 1 - lane % 2) for s in range(sets)]

    def permute(ref, index, rows):
        def step(m, carry):
            here = pl.ds(pl.multiple_of(m * cy, 8), cy)
            ref[here, :] = take(ref[here, :], index)
            return carry
        lax.fori_loop(0, rows // cy, step, 0, unroll=2 * UNROLL)

    def split(ref, x):
        a, b = ref[0, plain(x), :], ref[1, plain(x), :]
        return jnp.where(low, a, b), roll(jnp.where(low, b, a), HALF)

    def join(even_z, odd_z):
        turned = roll(odd_z, HALF)
        return jnp.where(low, even_z, turned), jnp.where(low, turned, even_z)

    def keep(e, x, pair):
        for k in range(2):
            ext[e, inner(k, x), :] = pair[k]

    def load(e, ref):
        def body(x):
            pair = split(ref, x)
            keep(e, x, pair)
            return pair, ()
        return sweep(body, 2 if e in DEEP else 1)[0]

    def load_kap(x):
        value = 4.0 * jnp.exp(-2.0 * lr_ref[plain(x), :])
        kap[plain(x), :] = value
        a = value + 6.0
        b = roll(a, HALF)
        pair = jnp.where(low, a, b), jnp.where(low, b, a)
        keep(KAP, x, pair)
        return pair, ()

    upper = lines // 2

    def observe(s):
        cell = idx_ref[s]
        value = val_ref[s]
        top = value.astype(jnp.bfloat16).astype(jnp.float32)
        line = cell // cz
        key = line // upper * LANES + cell % cz
        col = lax.broadcasted_iota(jnp.int32, (2 * LANES, nobs), 0)
        half = col % LANES // HALF
        hit = key == col // LANES * LANES + 2 * (col % HALF) + (half if s == 0 else 1 - half)
        for n, part in enumerate((1.0, top, value - top)):
            cols[2 * LANES * n:2 * LANES * (n + 1)] = jnp.where(hit, part, 0.0).astype(jnp.bfloat16)
        short = line % upper

        def step(m, carry):
            ids = lax.broadcasted_iota(jnp.int32, (upper, nobs), 0) + m * upper
            hot = jnp.where(ids == short, 1.0, 0.0).astype(jnp.bfloat16)
            got = lax.dot_general(hot, cols[...], (((1,), (1,)), ((), ())), preferred_element_type=jnp.float32)
            count = got[:, :2 * LANES] * (1.0 / noise_var)
            amount = (got[:, 2 * LANES:4 * LANES] + got[:, 4 * LANES:]) * (1.0 / noise_var)
            for h in range(2):
                here = pl.ds(pl.multiple_of(m * upper + h * upper, upper), upper)
                raw[s, 0, here, :] = count[:, h * LANES:(h + 1) * LANES]
                raw[s, 1, here, :] = amount[:, h * LANES:(h + 1) * LANES]
            return carry

        lax.fori_loop(0, 1, step, 0)

    loads[0].wait()
    for s in range(sets):
        permute(start_ref.at[s], apart[s], lines)
    faces_start = load(X0, start_ref)
    loads[3].wait()
    permute(lr_ref, apart[0], lines)
    faces_kap = sweep(load_kap, 1)[0]
    pl.semaphore_wait(barrier, total - 1)
    send_x(X0, faces_start)
    send(X0, faces_start)
    send_x(KAP)
    send(KAP, faces_kap)
    loads[4].wait()
    for s in range(sets):
        permute(state_ref.at[s], apart[s], lines)
    loads[1].wait()
    loads[2].wait()
    observe(0)
    observe(1)

    def right_pass(x):
        here = plain(x)
        counts = [raw[s, 0, here, :] for s in range(sets)]
        right = [raw[s, 1, here, :] - counts[s] * (state_ref[s, here, :] + start_ref[s, here, :]) for s in range(sets)]
        for ref, (a, b) in ((weight, counts), (rhs, right)):
            ref[dense(0, x), :] = jnp.where(low, a, b)
            ref[dense(1, x), :] = roll(jnp.where(low, b, a), HALF)
        return (None, None), ()

    sweep(right_pass)
    arrive(KAP)
    kz[...] = cp[PAD:]
    arrive(X0)
    near(X0)

    def residual_pass(x):
        out = again(X0, x)
        pair = [rhs[dense(k, x), :] - out[k] for k in range(2)]
        keep(R0, x, pair)
        return pair, ()

    send(R0, sweep(residual_pass, 2, early=R0, after=X0)[0])

    faces = load(STATE, state_ref)
    send_x(STATE)
    send(STATE, faces)

    arrive(R0)
    near(R0)

    def image_pass(x):
        out = again(R0, x)
        now = [ext[R0, inner(k, x), :] for k in range(2)]
        pair = [out[k] + weight[dense(k, x), :] * now[k] for k in range(2)]
        keep(W0, x, pair)
        return pair, (now[0] * now[0] + now[1] * now[1], now[0] * pair[0] + now[1] * pair[1])

    faces, gathered = sweep(image_pass, 2, 2, early=W0, after=R0)
    reduce_start(0, gathered)
    send(W0, faces)

    arrive(STATE)

    def state_pass(x):
        out = once(STATE, x)
        for k in range(2):
            ast[dense(k, x), :] = out[k]
        return (None, None), ()

    sweep(state_pass)

    norms, steps, ratios = [], [], []
    for k, e in enumerate((W0, W1)):
        arrive(e)
        near(e)
        norm, product = reduce_end(k)
        if k == 0:
            ratio, step_size = None, norm / product
        else:
            ratio = norm / norms[-1]
            step_size = norm / (product - ratio * norm / steps[-1])
        norms.append(norm)
        steps.append(step_size)
        ratios.append(ratio)

        def update(x, k=k, e=e, ratio=ratio, step_size=step_size):
            pair, terms, out = [], [], again(e, x)
            for p in range(2):
                here, there = dense(p, x), inner(p, x)
                vec = ext[e, there, :]
                image = out[p] + weight[here, :] * vec
                if k == 0:
                    z[here, :] = image
                    follow, now = vec, ext[R0, there, :]
                else:
                    image = image + ratio * z[here, :]
                    follow, now = vec + ratio * ext[W0, there, :], r[k - 1, here, :]
                    s_buf[here, :] = follow
                vec = vec - step_size * image
                now = now - step_size * follow
                ext[e + 1, there, :] = vec
                r[k, here, :] = now
                pair.append(vec)
                terms.append((now * now, now * vec))
            return pair, (terms[0][0] + terms[1][0], terms[0][1] + terms[1][1])

        faces, gathered = sweep(update, 2 if e + 1 in DEEP else 1, 2, early=e + 1, after=e)
        reduce_start(k + 1, gathered)
        send(e + 1, faces)

        def trail(x, k=k, ratio=ratio, step_size=step_size):
            for p in range(2):
                here, there = dense(p, x), inner(p, x)
                if k == 0:
                    xs[here, :] = ext[X0, there, :] + step_size * ext[R0, there, :]
                    now = uext[R0, there, :]
                    axs[here, :] = uext[X0, there, :] + step_size * now
                    ar[0, here, :] = now - step_size * uext[W0, there, :]
                else:
                    toward = r[0, here, :] + ratio * ext[R0, there, :]
                    rhs[here, :] = toward
                    xs[here, :] = xs[here, :] + step_size * toward
                    now = ar[0, here, :]
                    toward = now + ratio * uext[R0, there, :]
                    ad[here, :] = toward
                    axs[here, :] = axs[here, :] + step_size * toward
                    follow = uext[W1, there, :] + ratio * uext[W0, there, :]
                    q[here, :] = follow
                    ar[1, here, :] = now - step_size * follow
            return (None, None), ()

        sweep(trail)

    arrive(W2)

    def last_half(x):
        out = once(W2, x)
        for p in range(2):
            z[dense(p, x), :] = out[p]
        return (None, None), ()

    sweep(last_half)
    norm, product = reduce_end(2)
    ratio = norm / norms[-1]
    step_size = norm / (product - ratio * norm / steps[-1])

    def last_residual(x):
        norm_terms, terms = [], []
        for p in range(2):
            here, there = dense(p, x), inner(p, x)
            now = r[1, here, :] - step_size * (ext[W2, there, :] + ratio * s_buf[here, :])
            inner_now = ar[1, here, :] - step_size * (z[here, :] + ratio * q[here, :])
            r[2, here, :] = now
            ar[2, here, :] = inner_now
            norm_terms.append(now * now)
            terms.append(inner_now * inner_now + weight[here, :] * now * now)
        return (None, None), (norm_terms[0] + norm_terms[1], terms[0] + terms[1])

    reduce_start(3, sweep(last_residual, 0, 2)[1])

    def prepare(x):
        towards, olds, nows, grads = [], [], [], []
        for p in range(2):
            here, there = dense(p, x), inner(p, x)
            field, image = ext[STATE, there, :], ast[here, :]
            toward = r[1, here, :] + ratio * rhs[here, :]
            applied = ar[1, here, :] + ratio * ad[here, :]
            old = xs[here, :] + step_size * toward
            old_applied = axs[here, :] + step_size * applied
            now, now_applied = r[2, here, :], ar[2, here, :]
            towards.append(toward)
            olds.append(old)
            nows.append(now)
            grads.append((
                old * image + old_applied * field,
                now * image + now_applied * field,
                toward * image + applied * field,
            ))
        here = plain(x)
        scale = -2.0 * kap[here, :]
        for s, v in enumerate(join(*olds)):
            adj_ref[s, here, :] = v
        for n, pair in enumerate((nows, towards)):
            for s, v in enumerate(join(*pair)):
                raw[s, n, here, :] = v
        parts = [join(grads[0][n], grads[1][n]) for n in range(3)]
        grad_ref[here, :] = scale * (parts[0][0] + roll(parts[0][1], HALF))
        for s, factor in enumerate((scale, roll(scale, HALF))):
            gr[s, here, :] = factor * parts[1][s]
            gd[s, here, :] = factor * parts[2][s]
        return (None, None), ()

    sweep(prepare, unroll=4)
    for s in range(sets):
        for ref in (adj_ref.at[s], raw.at[s, 0], raw.at[s, 1], gr.at[s], gd.at[s]):
            permute(ref, together[s], lines)
    permute(grad_ref, together[0], lines)
    last_norm, last_product = reduce_end(3)
    last_ratio = last_norm / norm
    last_step = last_norm / (last_product - last_ratio * last_norm / step_size)
    last_both = last_step * last_ratio
    one = [spread(last_step, s * HALF) for s in range(sets)]
    two = [spread(last_both, s * HALF) for s in range(sets)]

    def finish(x, carry):
        here = plain(x)
        grad = grad_ref[here, :]
        for s in range(sets):
            adj_ref[s, here, :] = adj_ref[s, here, :] + (one[s] * raw[s, 0, here, :] + two[s] * raw[s, 1, here, :])
            grad = grad + (one[s] * gr[s, here, :] + two[s] * gd[s, here, :])
        grad_ref[here, :] = grad
        return carry
    stores = []
    for c in range(CHUNKS):
        lax.fori_loop(c * cx // CHUNKS, (c + 1) * cx // CHUNKS, finish, 0, unroll=True)
        part = slice(c * lines // CHUNKS, (c + 1) * lines // CHUNKS)
        targets = [(grad_ref.at[part], grad_hbm.at[part])]
        targets += [(adj_ref.at[s, part], adj_hbm.at[s, part]) for s in range(sets)]
        for n, (src, dst) in enumerate(targets):
            stores.append(pltpu.make_async_copy(src, dst, store_sem.at[c, n]))
            stores[-1].start()
    for copy in stores:
        copy.wait()


def hand_over(grad_in, adj_in, grad_out, adj_out, buf, in_sem, out_sem):
    sets, rows, _ = adj_in.shape
    half = rows // 2
    pairs = []
    for h in range(2):
        part = slice(h * half, (h + 1) * half)
        pairs.append((grad_in.at[part], grad_out.at[part]))
        pairs += [(adj_in.at[s, part], adj_out.at[s, part]) for s in range(sets)]
    loads = [pltpu.make_async_copy(a, buf.at[n], in_sem.at[n]) for n, (a, b) in enumerate(pairs)]
    stores = [pltpu.make_async_copy(buf.at[n], b, out_sem.at[n]) for n, (a, b) in enumerate(pairs)]
    for copy in loads:
        copy.start()
    for load, store in zip(loads, stores):
        load.wait()
        store.start()
    for copy in stores:
        copy.wait()


def on_device(sizes, log_range, state, adjoint_start, obs_index, obs_value):
    sets, cx, cy, cz = state.shape
    nobs = obs_index.shape[-1]
    rows = cx * cy
    total = sizes[0] * sizes[1] * sizes[2]
    whole = 2 * (cx + 2 * GHOST) * (cy + PAD) + 8
    f32 = jnp.float32
    field = pltpu.VMEM((2 * rows, LANES), f32)
    natural = pltpu.VMEM((sets, rows, cz), f32)
    hbm = pl.BlockSpec(memory_space=pltpu.HBM)
    gradient, adjoint = pl.pallas_call(
        functools.partial(kernel, sizes, (sets, cx, cy, cz, nobs)),
        out_shape=(
            jax.ShapeDtypeStruct((rows, cz), jnp.float32),
            jax.ShapeDtypeStruct((sets, rows, cz), jnp.float32),
        ),
        in_specs=[hbm] * 5,
        out_specs=(hbm, hbm),
        scratch_shapes=[
            pltpu.VMEM((rows, cz), f32),
            natural,
            pltpu.VMEM((rows, cz), f32),
            natural,
            natural,
            pltpu.VMEM((sets, 1, nobs), jnp.int32),
            pltpu.VMEM((sets, 1, nobs), f32),
            pltpu.VMEM((FIELDS, whole, LANES), f32),
            pltpu.VMEM((len(DEEP), whole, LANES), f32),
            pltpu.VMEM((FIELDS, 2, GHOST, 2 * cx, LANES), f32),
            pltpu.VMEM((FIELDS, 2, GHOST, 2 * cx, LANES), f32),
            pltpu.VMEM((FIELDS, 2, cy, LANES), f32),
            pltpu.VMEM((FIELDS, 2, cy + 2 * PAD, LANES), f32),
            pltpu.VMEM((FIELDS, cy, LANES), f32),
            *[pltpu.VMEM((len(DEEP), 4, 8, LANES), f32)] * 4,
            pltpu.VMEM((cy + 2 * PAD, LANES), f32),
            pltpu.VMEM((cy + PAD, LANES), f32),
            pltpu.VMEM((2, cy, LANES), f32),
            pltpu.VMEM((cy, LANES), f32),
            pltpu.VMEM((cy, LANES), f32),
            pltpu.VMEM((rows, cz), f32),
            pltpu.VMEM((6 * LANES, nobs), jnp.bfloat16),
            pltpu.VMEM((sets, 2, rows, LANES), f32),
            field, field, field, field,
            pltpu.VMEM((3, 2 * rows, LANES), f32),
            pltpu.VMEM((3, 2 * rows, LANES), f32),
            *[field] * 5,
            natural, natural,
            pltpu.VMEM((ITERS, 1, LANES), f32),
            pltpu.VMEM((ITERS, total, 1, LANES), f32),
            pltpu.SemaphoreType.DMA((FIELDS, COPIES)),
            pltpu.SemaphoreType.DMA((FIELDS, COPIES)),
            pltpu.SemaphoreType.DMA((ITERS,)),
            pltpu.SemaphoreType.DMA((ITERS,)),
            pltpu.SemaphoreType.DMA((5,)),
            pltpu.SemaphoreType.DMA((CHUNKS, 1 + sets)),
        ],
        compiler_params=pltpu.CompilerParams(
            collective_id=0, has_side_effects=True, vmem_limit_bytes=63 * 1024 * 1024
        ),
    )(
        log_range.reshape(rows, cz),
        state.reshape(sets, rows, cz),
        adjoint_start.reshape(sets, rows, cz),
        obs_index.reshape(sets, 1, nobs),
        obs_value.reshape(sets, 1, nobs),
    )
    gradient, adjoint = pl.pallas_call(
        hand_over,
        out_shape=(
            jax.ShapeDtypeStruct((rows, cz), jnp.float32),
            jax.ShapeDtypeStruct((sets, rows, cz), jnp.float32),
        ),
        in_specs=[hbm] * 2,
        out_specs=(hbm, hbm),
        scratch_shapes=[
            pltpu.VMEM((2 + 2 * sets, rows // 2, cz), f32),
            pltpu.SemaphoreType.DMA((2 + 2 * sets,)),
            pltpu.SemaphoreType.DMA((2 + 2 * sets,)),
        ],
    )(gradient, adjoint)
    return gradient.reshape(cx, cy, cz), adjoint.reshape(sets, cx, cy, cz)


def solution(mesh):
    in_specs = (
        P("gx", "gy", "gz"),
        P(None, "gx", "gy", "gz"),
        P(None, "gx", "gy", "gz"),
        P(None, "gx", "gy", "gz", None),
        P(None, "gx", "gy", "gz", None),
    )
    out_specs = (P("gx", "gy", "gz"), P(None, "gx", "gy", "gz"))
    sizes = tuple(mesh.shape[axis] for axis in AXES)
    return jax.shard_map(
        functools.partial(on_device, sizes), mesh=mesh, in_specs=in_specs, out_specs=out_specs, check_vma=False
    )
```
